8 devices in a mesh: dp: 1 (over z), rep: 2 (over y), team: 4 (over x, core).
Axes of the slice: x: 2, y: 2, z: 1, core: 2. Of those that a mesh axis runs over, the one named last changes fastest.
Arguments:
- points: bfloat16 [8192, 90], P(('dp', 'team', 'rep'))
- values: bfloat16 [8192, 1], P(('dp', 'team', 'rep'))
- pair_mask: int32 [4, 4], P('dp')
- bandwidth: float32 [1], replicated
Outputs:
- output: float32 [8192, 1], P(('dp', 'team', 'rep'))
All inputs are finite; a program needn't handle non-finite values.
Results may differ from the reference program's by a relative error of at most 0.00585081.
Values are sent between devices in bfloat16 or wider.
A program may use at most 1 GiB of HBM per device.

```python
import jax
import jax.numpy as jnp
from jax import lax

ROWS = 1024
TEAM = 4
REP = 2
DIM = 90
RHS = 1
POINTS = ROWS * TEAM * REP
BLOCK = ROWS * REP


def setup_inputs(seed: int = 0, part: int = 0) -> dict:
    base_key, shared_key = jax.random.split(jax.random.key(seed))
    part_key = jax.random.fold_in(base_key, part)
    key_pts, key_vals, key_mask = jax.random.split(part_key, 3)
    points = jax.random.normal(key_pts, (POINTS, DIM), jnp.float32).astype(jnp.bfloat16)
    values = (jax.random.normal(key_vals, (POINTS, RHS), jnp.float32) * POINTS ** -0.5).astype(jnp.bfloat16)
    team_ids = jnp.arange(TEAM)
    mask_draw = jax.random.randint(key_mask, (TEAM, TEAM), 0, 4)
    draw_sym = jnp.where(team_ids[:, None] < team_ids[None, :], mask_draw, mask_draw.T)
    must_keep = (team_ids[:, None] == team_ids[None, :]) | (team_ids[:, None] == 0) | (team_ids[None, :] == 0)
    pair_mask = jnp.where(must_keep, jnp.maximum(draw_sym, 1), draw_sym).astype(jnp.int32)
    bandwidth = DIM * jax.random.uniform(shared_key, (1,), jnp.float32, minval=0.7, maxval=1.3)
    return {"points": points, "values": values, "pair_mask": pair_mask, "bandwidth": bandwidth}


def reference(points, values, pair_mask, bandwidth):
    width = bandwidth[0]
    sq_norm = jnp.sum(jnp.square(points.astype(jnp.float32)), axis=1)
    key_pts = points.reshape(TEAM, BLOCK, DIM)
    key_vals = values.reshape(TEAM, BLOCK, RHS)
    key_sq = sq_norm.reshape(TEAM, BLOCK)
    mask_cols = pair_mask.astype(jnp.float32).T
    query_pts = points.reshape(TEAM * REP, ROWS, DIM)
    query_sq = sq_norm.reshape(TEAM * REP, ROWS)
    query_team = jnp.arange(TEAM * REP) // REP

    def one_query(item):
        q_points, q_sq, team_id = item

        def over_keys(total, key_item):
            k_points, k_values, k_sq, weight_col = key_item
            cross_dot = jnp.dot(q_points, k_points.T, preferred_element_type=jnp.float32)
            sq_dist = q_sq[:, None] + k_sq[None, :] - 2.0 * cross_dot
            kernel = jnp.exp(-sq_dist / width).astype(jnp.bfloat16)
            total = total + weight_col[team_id] * jnp.dot(kernel, k_values, preferred_element_type=jnp.float32)
            return total, None

        zero_sum = jnp.zeros((ROWS, RHS), jnp.float32)
        total, _ = lax.scan(over_keys, zero_sum, (key_pts, key_vals, key_sq, mask_cols))
        return total

    field = lax.map(one_query, (query_pts, query_sq, query_team))
    return field.reshape(POINTS, RHS)
```

```python
import functools

import jax
import jax.numpy as jnp
from jax import lax
from jax.experimental import pallas as pl
from jax.experimental.pallas import tpu as pltpu
from jax.sharding import PartitionSpec as P

MESH = pl.DeviceIdType.MESH
N = 1024
SUB = 256
LOG2E = 1.4426950408889634


def chunks(sizes):
    out, at = [], 0
    for size in sizes:
        out.append((at, size))
        at += size
    return out


C1 = chunks((512, 512))
C3 = chunks((512, 256, 256))
NK = 4


def split3(s):
    hi = s.astype(jnp.bfloat16).astype(jnp.float32)
    rest = s - hi
    mid = rest.astype(jnp.bfloat16).astype(jnp.float32)
    return hi, mid, rest - mid


def augment(xt, weights):
    n = xt.shape[1]
    x32 = xt.astype(jnp.float32)
    hi, mid, lo = split3(jnp.sum(x32 * x32, axis=0, keepdims=True))
    last = jnp.concatenate([x32[80:90], jnp.zeros((6, n), jnp.float32)], axis=0)
    row = lax.broadcasted_iota(jnp.int32, (16, n), 0)
    if weights:
        tail = jnp.where(row < 10, -2.0 * last, jnp.where(row < 13, 1.0, jnp.where(row == 13, hi, jnp.where(row == 14, mid, lo))))
        return jnp.concatenate([(-2.0 * x32[:80]).astype(jnp.bfloat16), tail.astype(jnp.bfloat16)], axis=0)
    tail = jnp.where(row < 10, last, jnp.where(row >= 13, 1.0, jnp.where(row == 10, hi, jnp.where(row == 11, mid, lo))))
    return jnp.concatenate([xt[:80], tail.astype(jnp.bfloat16)], axis=0)


def kernel(x_hbm, v_hbm, m_hbm, h_ref, o_ref, xb, vb, mb, wb, lb, fb, load_sem, send_sem, recv_sem, vsend_sem, vrecv_sem):
    y, t, dp = lax.axis_index("rep"), lax.axis_index("team"), lax.axis_index("dp")
    x, c = t // 2, t % 2

    def dev(dx, dy, dc):
        return (dp, y + dy - 2 * y * dy, 2 * (x + dx - 2 * x * dx) + c + dc - 2 * c * dc)

    partner, target, source, across = dev(0, 0, 1), dev(1 - c, c, 1), dev(c, 1 - c, 1), dev(1, 0, 0)
    third = dev(1 - c, c, c)

    bar = pltpu.get_barrier_semaphore()
    for d in (partner, source, across):
        pl.semaphore_signal(bar, inc=1, device_id=d, device_id_type=MESH)
    loads = [pltpu.make_async_copy(src, dst, load_sem.at[i]) for i, (src, dst) in enumerate(((x_hbm, xb.at[0]), (v_hbm, vb.at[0]), (m_hbm, mb)))]
    for z in loads:
        z.start()
    wb[96:256, :] = jnp.zeros((160, N), jnp.bfloat16)
    lb[...] = jnp.zeros_like(lb)

    sends = []

    def remote(src, dst, ssem, rsem, d):
        return pltpu.make_async_remote_copy(src_ref=src, dst_ref=dst, send_sem=ssem, recv_sem=rsem, device_id=d, device_id_type=MESH)

    def send_x(src, slot, at, k, lane, d):
        cols = pl.ds(at[0], at[1])
        z = remote(src.at[:, cols], xb.at[slot, :, cols], send_sem.at[lane, k], recv_sem.at[slot, k], d)
        z.start()
        return z

    def send_v(src, slot, lane, d):
        z = remote(src, vb.at[slot], vsend_sem.at[lane], vrecv_sem.at[slot], d)
        z.start()
        return z

    def recv_x(slot, at, k):
        ref = xb.at[slot, :, pl.ds(at[0], at[1])]
        remote(ref, ref, send_sem.at[0, k], recv_sem.at[slot, k], partner).wait_recv()

    def recv_v(slot):
        remote(vb.at[slot], vb.at[slot], vsend_sem.at[0], vrecv_sem.at[slot], partner).wait_recv()

    def compute(accs):
        fb[...] = jnp.zeros_like(fb)
        pl.semaphore_wait(bar, 3)
        sends.append(send_v(v_hbm, 5 + c, 0, target))
        for k, at in enumerate(C1):
            sends.append(send_x(x_hbm, 5 + c, at, k, 0, target))
        sends.append(send_v(v_hbm, 4, 1, partner))
        for k, at in enumerate(C1):
            sends.append(send_x(x_hbm, 4, at, k, 1, partner))
        loads[0].wait()
        loads[1].wait()
        alpha = -LOG2E / h_ref[0]
        for i in range(0, N, SUB):
            wb[0:96, i:i + SUB] = augment(xb[0, :, i:i + SUB], True)

        state = dict(ring=0, buf=0, pend=[])
        rows = lax.broadcasted_iota(jnp.int32, (16, SUB), 0)

        def flush(keep=0):
            pass

        def tiles(slot, team, at):
            r = state["ring"]
            state["ring"] = (r + 1) % 4
            size = at[1]
            lhs = augment(xb[slot, :, at[0]:at[0] + size], False).T
            rows = lax.broadcasted_iota(jnp.int32, (16, size), 0)
            vv = jnp.where(rows == team, jnp.broadcast_to(vb[slot, :, at[0]:at[0] + size].astype(jnp.float32), (16, size)), 0.0).astype(jnp.bfloat16)
            d = jnp.dot(lhs, wb[0:96, :], preferred_element_type=jnp.float32)
            kern = jnp.exp2(d * alpha).astype(jnp.bfloat16)
            fb[...] += jnp.dot(vv, kern, preferred_element_type=jnp.float32)

        def team_of(dx, dc):
            return 2 * (x + dx - 2 * x * dx) + c + dc - 2 * c * dc

        f1, f2, p1, p2 = 6 - c, 2 - c, 1 + c, 5 + c
        T = dict(own=team_of(0, 0), part=team_of(0, 1), f1=team_of(c, 1), p1=team_of(1 - c, 0), f2=team_of(c, 0), p2=team_of(1 - c, 1), d3=team_of(1, 0), d7=team_of(1, 1))
        whole = (0, N)

        tiles(0, T["own"], whole)
        flush()
        recv_v(4)
        sends.append(send_v(vb.at[4], 1 + c, 2, target))
        for k, at in enumerate(C1):
            recv_x(4, at, k)
            sends.append(send_x(xb.at[4], 1 + c, at, k, 2, target))
        tiles(4, T["part"], whole)
        flush()

        cond_sends = []
        nk = len(C1)
        later = []
        recv_v(f1)
        for k, at in enumerate(C1):
            recv_x(f1, at, k)
            if k == 0:
                sends.append(send_v(vb.at[f1], 7 - 4 * c, 3, third))
                sends.append(send_v(vb.at[f1], 2 - c, 4, partner))
            sends.append(send_x(xb.at[f1], 2 - c, at, k, 4, partner))
            for k3, at3 in enumerate(C3):
                if at[0] < at3[0] + at3[1] <= at[0] + at[1]:
                    sends.append(send_x(xb.at[f1], 7 - 4 * c, at3, k3, 3, third))
            tiles(f1, T["f1"], at)
            if k > 0:
                recv_x(p1, C1[k - 1], k - 1)
                if k == 1:
                    recv_v(p1)
                tiles(p1, T["p1"], C1[k - 1])
            flush()
        recv_v(f2)
        sends.append(send_v(vb.at[f2], 6 - c, 5, partner))
        for k, at in enumerate(C1):
            recv_x(f2, at, k)
            sends.append(send_x(xb.at[f2], 6 - c, at, k, 5, partner))
            tiles(f2, T["f2"], at)
            if k == 0:
                recv_x(p1, C1[-1], nk - 1)
                if nk == 1:
                    recv_v(p1)
                tiles(p1, T["p1"], C1[-1])
            else:
                recv_x(p2, C1[k - 1], k - 1)
                if k == 1:
                    recv_v(p2)
                tiles(p2, T["p2"], C1[k - 1])
            flush()
        recv_x(p2, C1[-1], nk - 1)
        if nk == 1:
            recv_v(p2)
        tiles(p2, T["p2"], C1[-1])
        flush()
        for k, at in enumerate(C3):
            recv_x(3, at, k)
            recv_x(7, at, k)
            if k == 0:
                recv_v(3)
                recv_v(7)

            @pl.when(c == 0)
            def _():
                if k == 0:
                    send_v(vb.at[3], 7, 6, partner)
                    send_v(vb.at[7], 3, 7, partner)
                send_x(xb.at[3], 7, at, k, 6, partner)
                send_x(xb.at[7], 3, at, k, 7, partner)

            tiles(3, T["d3"], at)
            tiles(7, T["d7"], at)
            flush()

        loads[2].wait()
        weight = jnp.sum(jnp.where(lax.broadcasted_iota(jnp.int32, (4, 4), 1) == t, mb[...].astype(jnp.float32), 0.0), axis=1, keepdims=True)
        o_ref[...] = jnp.sum(fb[0:4] * weight, axis=0, keepdims=True)

        for z in sends:
            z.wait_send()

        @pl.when(c == 0)
        def _():
            for k, at in enumerate(C3):
                cols = pl.ds(at[0], at[1])
                for s, lane in ((3, 6), (7, 7)):
                    remote(xb.at[s, :, cols], xb.at[10 - s, :, cols], send_sem.at[lane, k], recv_sem.at[10 - s, k], partner).wait_send()
            for s, lane in ((3, 6), (7, 7)):
                remote(vb.at[s], vb.at[10 - s], vsend_sem.at[lane], vrecv_sem.at[10 - s], partner).wait_send()

    compute(None)


def solution(mesh):
    spec = P(("dp", "team", "rep"), None)

    def per_device(points, values, pair_mask, bandwidth):
        hbm = [pltpu.with_memory_space_constraint(z, pltpu.HBM) for z in (points.T, values.T, pair_mask)]
        field = pl.pallas_call(
            kernel,
            out_shape=jax.ShapeDtypeStruct((1, N), jnp.float32),
            in_specs=[pl.BlockSpec(memory_space=pltpu.HBM)] * 3 + [pl.BlockSpec(memory_space=pltpu.SMEM)],
            out_specs=pl.BlockSpec(memory_space=pltpu.VMEM),
            scratch_shapes=[
                pltpu.VMEM((8, 90, N), jnp.bfloat16),
                pltpu.VMEM((8, 1, N), jnp.bfloat16),
                pltpu.VMEM((4, 4), jnp.int32),
                pltpu.VMEM((256, N), jnp.bfloat16),
                pltpu.VMEM((4, SUB, 256), jnp.bfloat16),
                pltpu.VMEM((16, N), jnp.float32),
                pltpu.SemaphoreType.DMA((3,)),
                pltpu.SemaphoreType.DMA((8, NK)),
                pltpu.SemaphoreType.DMA((8, NK)),
                pltpu.SemaphoreType.DMA((8,)),
                pltpu.SemaphoreType.DMA((8,)),
            ],
            compiler_params=pltpu.CompilerParams(collective_id=0, has_side_effects=True, vmem_limit_bytes=16 * 2**20),
        )(*hbm, bandwidth)
        return field.T

    return jax.shard_map(per_device, mesh=mesh, in_specs=(spec, spec, P("dp", None), P()), out_specs=spec, check_vma=False)
```

```python
import functools

import jax
import jax.numpy as jnp
from jax import lax
from jax.experimental import pallas as pl
from jax.experimental.pallas import tpu as pltpu
from jax.sharding import PartitionSpec as P

MESH = pl.DeviceIdType.MESH
N = 1024
SUB = 256
LOG2E = 1.4426950408889634


def chunks(sizes):
    out, at = [], 0
    for size in sizes:
        out.append((at, size))
        at += size
    return out


C1 = chunks((512, 512))
C3 = chunks((512, 512))
NK = 4
NOW = 0
TF = 0
NOV = 0
NOCOMP = 0
TJ = 256
TI = 512
LAG = 2
MERGE = 0


def split3(s):
    hi = s.astype(jnp.bfloat16).astype(jnp.float32)
    rest = s - hi
    mid = rest.astype(jnp.bfloat16).astype(jnp.float32)
    return hi, mid, rest - mid


def augment(xt, weights):
    n = xt.shape[1]
    x32 = xt.astype(jnp.float32)
    hi, mid, lo = split3(jnp.sum(x32 * x32, axis=0, keepdims=True))
    last = jnp.concatenate([x32[80:90], jnp.zeros((6, n), jnp.float32)], axis=0)
    row = lax.broadcasted_iota(jnp.int32, (16, n), 0)
    if weights:
        tail = jnp.where(row < 10, -2.0 * last, jnp.where(row < 13, 1.0, jnp.where(row == 13, hi, jnp.where(row == 14, mid, lo))))
        return jnp.concatenate([(-2.0 * x32[:80]).astype(jnp.bfloat16), tail.astype(jnp.bfloat16)], axis=0)
    tail = jnp.where(row < 10, last, jnp.where(row >= 13, 1.0, jnp.where(row == 10, hi, jnp.where(row == 11, mid, lo))))
    return jnp.concatenate([xt[:80], tail.astype(jnp.bfloat16)], axis=0)


def kernel(x_hbm, v_hbm, m_hbm, h_ref, o_ref, xb, vb, mb, wb, fb, load_sem, send_sem, recv_sem, vsend_sem, vrecv_sem, ready, peer, go):
    y, t, dp = lax.axis_index("rep"), lax.axis_index("team"), lax.axis_index("dp")
    x, c = t // 2, t % 2

    def dev(dx, dy, dc):
        return (dp, y + dy - 2 * y * dy, 2 * (x + dx - 2 * x * dx) + c + dc - 2 * c * dc)

    dx = c + y - 2 * c * y
    partner, target, source = dev(0, 0, 1), dev(dx, 1 - dx, dx), dev(1 - dx, dx, 1 - dx)

    last_chip = x * y
    bar = pltpu.get_barrier_semaphore()

    @pl.when(y * (1 - c * (1 - x)) == 0)
    def _():
        pl.semaphore_signal(bar, inc=1, device_id=source, device_id_type=MESH)

    @pl.when(c == 1)
    def _():
        pl.semaphore_signal(bar, inc=1, device_id=partner, device_id_type=MESH)

    loads = [pltpu.make_async_copy(src, dst, load_sem.at[i]) for i, (src, dst) in enumerate(((x_hbm, xb.at[0]), (v_hbm, vb.at[0]), (m_hbm, mb)))]
    for z in loads:
        z.start()

    sends = []

    def remote(src, dst, ssem, rsem, d):
        return pltpu.make_async_remote_copy(src_ref=src, dst_ref=dst, send_sem=ssem, recv_sem=rsem, device_id=d, device_id_type=MESH)

    def send_x(src, slot, at, k, lane, d, start=True):
        cols = pl.ds(at[0], at[1])
        z = remote(src.at[:, cols], xb.at[slot, :, cols], send_sem.at[lane, k], recv_sem.at[slot, k], d)
        if start:
            z.start()
        return z

    def send_v(src, slot, lane, d, start=True):
        z = remote(src, vb.at[slot], vsend_sem.at[lane], vrecv_sem.at[slot], d)
        if NOV:
            return None
        if start:
            z.start()
        return z

    def recv_x(slot, at, k):
        ref = xb.at[slot, :, pl.ds(at[0], at[1])]
        remote(ref, ref, send_sem.at[0, k], recv_sem.at[slot, k], partner).wait_recv()

    def recv_v(slot):
        if not NOV:
            remote(vb.at[slot], vb.at[slot], vsend_sem.at[0], vrecv_sem.at[slot], partner).wait_recv()

    def compute(accs):
        fb[...] = jnp.zeros_like(fb)
        def tiles(*parts):
            total, pend = {}, []
            ctx = jax.named_scope('tiles'); ctx.__enter__()
            if NOCOMP == 1 or (NOCOMP == 2 and parts[-1][0] != 7) or (NOCOMP==3 and parts[-1][0]==7):
                ctx.__exit__(None, None, None); return

            def drain():
                i, vv, d = pend.pop(0)
                kern = jnp.exp2(d * alpha).astype(jnp.bfloat16)
                r = jnp.dot(vv, kern, preferred_element_type=jnp.float32)
                total[i] = total[i] + r if i in total else r

            for slot, team, at in parts:
                lhs = augment(xb[slot, :, at[0]:at[0] + at[1]], False).T
                for j in range(0, at[1], TJ):
                    rows = lax.broadcasted_iota(jnp.int32, (16, TJ), 0)
                    v32 = vb[slot, :, at[0] + j:at[0] + j + TJ].astype(jnp.float32)
                    vv = jnp.where(rows == team, jnp.broadcast_to(v32, (16, TJ)), 0.0).astype(jnp.bfloat16)
                    for i in range(0, N, TI):
                        pend.append((i, vv, jnp.dot(lhs[j:j + TJ], wb[0:96, i:i + TI], preferred_element_type=jnp.float32)))
                        if len(pend) > LAG:
                            drain()
            while pend:
                drain()
            for i in total:
                fb[:, i:i + TI] += total[i]
            ctx.__exit__(None, None, None)

        def team_of(dx, dc):
            return 2 * (x + dx - 2 * x * dx) + c + dc - 2 * c * dc

        f1, f2, p1, p2 = 5 - 3 * dx, 1 + 5 * dx, 6 - 5 * dx, 2 + 3 * dx
        T = dict(own=team_of(0, 0), part=team_of(0, 1), f1=team_of(1 - dx, 1 - dx), f2=team_of(1 - dx, dx), p1=team_of(dx, 1 - dx), p2=team_of(dx, dx), d3=team_of(1, 0), d7=team_of(1, 1))

        def arrive(slot, k, ats, name='?'):
          with jax.named_scope(f'{name}{k}'):
            if k == 0:
                recv_v(slot)
            recv_x(slot, ats[k], k)

        def pass_on(slot, to, k, lane, d, ats):
            if k == 0:
                sends.append(send_v(vb.at[slot], to, lane, d))
            sends.append(send_x(xb.at[slot], to, ats[k], k, lane, d))

        n1, n3 = len(C1), len(C3)

        def got_first(k):
            arrive(f1, k, C1, 'f1_')
            end = C1[k][0] + C1[k][1]
            pass_on(f1, 1 + 5 * dx, k, 4, partner, C1)
            for k3, at3 in enumerate(C3):
                if C1[k][0] < at3[0] + at3[1] <= end:
                    pass_on(f1, 7, k3, 3, target, C3)
            return f1, T["f1"], C1[k]

        def got_second(k):
            arrive(f2, k, C1, 'f2_')
            pass_on(f2, 5 - 3 * dx, k, 5, partner, C1)
            return f2, T["f2"], C1[k]

        def got_p1(k):
            arrive(p1, k, C1, 'p1_')
            return p1, T["p1"], C1[k]

        def got_p2(k):
            arrive(p2, k, C1, 'p2_')
            return p2, T["p2"], C1[k]

        def got_third(k):
            arrive(7, k, C3, 'd7_')
            pass_on(7, 3, k, 6, partner, C3)
            return 7, T["d7"], C3[k]

        def got_last(k):
            arrive(3, k, C3, 'd3_')
            return 3, T["d3"], C3[k]

        alpha = -LOG2E / h_ref[0]

        def prepare():
            loads[0].wait()
            loads[1].wait()
            loads[2].wait()
            for i in range(0, N, SUB):
                wb[0:96, i:i + SUB] = augment(xb[0, :, i:i + SUB], True)

        first_chip = (1 - x) * (1 - y)

        @pl.when(first_chip == 1)
        def _():
            prepare()
            tiles((0, T["own"], (0, N)))

        with jax.named_scope('bar'):
            pl.semaphore_wait(bar, 1 + last_chip * (1 - c))

        def own_to_link(start):
            for k, at in enumerate(C1):
                z = send_x(x_hbm, 2 + 3 * dx, at, k, 0, target, start)
                zv = send_v(v_hbm, 2 + 3 * dx, 0, target, start) if k == 0 else None
                if not start:
                    z.wait_send()
                    if zv is not None:
                        zv.wait_send()

        direct = jnp.maximum(c, last_chip)

        @pl.when(direct == 1)
        def _():
            own_to_link(True)

        @pl.when(c == 0)
        def _():
            pl.semaphore_signal(ready, inc=1, device_id=partner, device_id_type=MESH)

        @pl.when(c == 1)
        def _():
            pl.semaphore_wait(ready, 1)

        @pl.when(y * (1 - (1 - x) * (1 - c)) == 1)
        def _():
            pl.semaphore_signal(peer, inc=1, device_id=target, device_id_type=MESH)

        for k, at in enumerate(C1):
            sends.append(send_x(x_hbm, 4, at, k, 1, partner))
        sends.append(send_v(v_hbm, 4, 1, partner))
        @pl.when(first_chip == 0)
        def _():
            prepare()

        @pl.when(c * (1 - last_chip) == 1)
        def _():
            with jax.named_scope('peer'):
                pl.semaphore_wait(peer, 1)
            pl.semaphore_signal(go, inc=1, device_id=partner, device_id_type=MESH)

        @pl.when(direct == 0)
        def _():
            with jax.named_scope('go'):
                pl.semaphore_wait(go, 1)
            own_to_link(True)

        for k in range(n1):
            arrive(4, k, C1, 'own4_')
            pass_on(4, 6 - 5 * dx, k, 2, target, C1)

        @pl.when(first_chip == 0)
        def _():
            tiles((0, T["own"], (0, N)))

        tiles((4, T["part"], (0, N)))
        weight = jnp.sum(jnp.where(lax.broadcasted_iota(jnp.int32, (4, 4), 1) == t, mb[...].astype(jnp.float32), 0.0), axis=1, keepdims=True)
        events = [[(got_first, 0)]]
        queue = [(got_first, k) for k in range(1, n1)] + [(got_second, k) for k in range(n1)]
        behind = [(got_p1, k) for k in range(n1)] + [(got_p2, k) for k in range(n1)]
        while queue:
            events.append([queue.pop(0), behind.pop(0)])
        events.append([behind.pop(0)])
        tail = ['70','71','30','31']
        for g in tail:
            events.append([((got_third if g[m] == '7' else got_last), int(g[m + 1])) for m in range(0, len(g), 2)])
        for group in events:
            parts = []
            for got, k in group:
                r = got(k)
                parts += r if isinstance(r[0], tuple) else [r]
            tiles(*parts)

        o_ref[...] = jnp.sum(fb[0:4] * weight, axis=0, keepdims=True)

        own_to_link(False)
        with jax.named_scope('sendw'):
          for z in sends:
            if z is not None:
                z.wait_send()

    compute(None)


def solution(mesh):
    spec = P(("dp", "team", "rep"), None)

    def per_device(points, values, pair_mask, bandwidth):
        hbm = [pltpu.with_memory_space_constraint(z, pltpu.HBM) for z in (points.T, values.T, pair_mask)]
        field = pl.pallas_call(
            kernel,
            out_shape=jax.ShapeDtypeStruct((1, N), jnp.float32),
            in_specs=[pl.BlockSpec(memory_space=pltpu.HBM)] * 3 + [pl.BlockSpec(memory_space=pltpu.SMEM)],
            out_specs=pl.BlockSpec(memory_space=pltpu.VMEM),
            scratch_shapes=[
                pltpu.VMEM((8, 90, N), jnp.bfloat16),
                pltpu.VMEM((8, 1, N), jnp.bfloat16),
                pltpu.VMEM((4, 4), jnp.int32),
                pltpu.VMEM((96, N), jnp.bfloat16),
                pltpu.VMEM((16, N), jnp.float32),
                pltpu.SemaphoreType.DMA((3,)),
                pltpu.SemaphoreType.DMA((8, NK)),
                pltpu.SemaphoreType.DMA((8, NK)),
                pltpu.SemaphoreType.DMA((8,)),
                pltpu.SemaphoreType.DMA((8,)),
                pltpu.SemaphoreType.REGULAR,
                pltpu.SemaphoreType.REGULAR,
                pltpu.SemaphoreType.REGULAR,
            ],
            compiler_params=pltpu.CompilerParams(collective_id=0, has_side_effects=True, vmem_limit_bytes=16 * 2**20),
        )(*hbm, bandwidth)
        return field.T

    return jax.shard_map(per_device, mesh=mesh, in_specs=(spec, spec, P("dp", None), P()), out_specs=spec, check_vma=False)
```

```python
import functools

import jax
import jax.numpy as jnp
from jax import lax
from jax.experimental import pallas as pl
from jax.experimental.pallas import tpu as pltpu
from jax.sharding import PartitionSpec as P

MESH = pl.DeviceIdType.MESH
N = 1024
LOG2E = 1.4426950408889634
TJ = 256
TI = 512
LAG = 3
SCOPED = 1
NOCOMP = 0
HALVES = ((0, 512), (512, 512))


def split3(s):
    hi = s.astype(jnp.bfloat16).astype(jnp.float32)
    rest = s - hi
    mid = rest.astype(jnp.bfloat16).astype(jnp.float32)
    return hi, mid, rest - mid


def augment(xt, weights):
    n = xt.shape[1]
    x32 = xt.astype(jnp.float32)
    hi, mid, lo = split3(jnp.sum(x32 * x32, axis=0, keepdims=True))
    last = jnp.concatenate([x32[80:90], jnp.zeros((6, n), jnp.float32)], axis=0)
    row = lax.broadcasted_iota(jnp.int32, (16, n), 0)
    if weights:
        tail = jnp.where(row < 10, -2.0 * last, jnp.where(row < 13, 1.0, jnp.where(row == 13, hi, jnp.where(row == 14, mid, lo))))
        return jnp.concatenate([(-2.0 * x32[:80]).astype(jnp.bfloat16), tail.astype(jnp.bfloat16)], axis=0)
    tail = jnp.where(row < 10, last, jnp.where(row >= 13, 1.0, jnp.where(row == 10, hi, jnp.where(row == 11, mid, lo))))
    return jnp.concatenate([xt[:80], tail.astype(jnp.bfloat16)], axis=0)


def body(x_hbm, v_hbm, m_hbm, h_ref, o_ref, xb, vb, mb, wb, fb, load_sem, sent_x, sent_v, got_x, got_v, note, peer):
    y, t, dp = lax.axis_index("rep"), lax.axis_index("team"), lax.axis_index("dp")
    x, c = t // 2, t % 2
    dx = c + y - 2 * c * y
    odd = x + y - 2 * x * y
    first_chip, last_chip = (1 - x) * (1 - y), x * y

    def dev(fx, fy, fc):
        return (dp, y + fy - 2 * y * fy, 2 * (x + fx - 2 * x * fx) + c + fc - 2 * c * fc)

    def team_of(fx, fc):
        return 2 * (x + fx - 2 * x * fx) + c + fc - 2 * c * fc

    partner, target, source = dev(0, 0, 1), dev(dx, 1 - dx, dx), dev(1 - dx, dx, 1 - dx)

    def signal(sem, d):
        pl.semaphore_signal(sem, inc=1, device_id=d, device_id_type=MESH)

    bar = pltpu.get_barrier_semaphore()
    pl.when(last_chip == 0)(lambda: signal(bar, source))
    pl.when(jnp.maximum(c, 1 - odd) == 1)(lambda: signal(bar, partner))
    loads = [pltpu.make_async_copy(src, dst, load_sem.at[i]) for i, (src, dst) in enumerate(((x_hbm, xb.at[0]), (v_hbm, vb.at[0]), (m_hbm, mb)))]
    for z in loads:
        z.start()
    fb[...] = jnp.zeros_like(fb)

    def copy_x(src, dst, slot, k, d):
        return pltpu.make_async_remote_copy(src_ref=src, dst_ref=dst, send_sem=sent_x, recv_sem=got_x.at[slot - 1, k], device_id=d, device_id_type=MESH)

    def copy_v(src, slot, d):
        return pltpu.make_async_remote_copy(src_ref=src, dst_ref=vb.at[slot], send_sem=sent_v, recv_sem=got_v.at[slot - 1], device_id=d, device_id_type=MESH)

    def send(x_src, v_src, slot, k, d):
        cols = pl.ds(*HALVES[k])
        copy_x(x_src.at[:, cols], xb.at[slot, :, cols], slot, k, d).start()
        if k == 0:
            copy_v(v_src, slot, d).start()

    def pass_on(slot, to, k, d):
        send(xb.at[slot], vb.at[slot], to, k, d)

    def arrive(slot, k, name):
        with jax.named_scope(f"{name}{k}"):
            if k == 0:
                copy_v(vb.at[slot], slot, partner).wait_recv()
            ref = xb.at[slot, :, pl.ds(*HALVES[k])]
            copy_x(ref, ref, slot, k, partner).wait_recv()

    alpha = -LOG2E / h_ref[0]

    def tiles(*parts):
        if NOCOMP:
            return
        total, pend = {}, []

        def drain():
            i, vv, d = pend.pop(0)
            kern = jnp.exp2(d * alpha).astype(jnp.bfloat16)
            r = jnp.dot(vv, kern, preferred_element_type=jnp.float32)
            total[i] = total[i] + r if i in total else r

        with jax.named_scope("tiles"):
            for slot, team, at in parts:
                lhs = augment(xb[slot, :, at[0]:at[0] + at[1]], False).T
                for j in range(0, at[1], TJ):
                    rows = lax.broadcasted_iota(jnp.int32, (16, TJ), 0)
                    v32 = vb[slot, :, at[0] + j:at[0] + j + TJ].astype(jnp.float32)
                    vv = jnp.where(rows == team, jnp.broadcast_to(v32, (16, TJ)), 0.0).astype(jnp.bfloat16)
                    for i in range(0, N, TI):
                        pend.append((i, vv, jnp.dot(lhs[j:j + TJ], wb[:, i:i + TI], preferred_element_type=jnp.float32)))
                        if len(pend) > LAG:
                            drain()
            while pend:
                drain()
            for i in total:
                fb[:, i:i + TI] += total[i]

    def prepare():
        for z in loads:
            z.wait()
        for i in range(0, N, 256):
            wb[:, i:i + 256] = augment(xb[0, :, i:i + 256], True)

    def own_sum():
        tiles((0, team_of(0, 0), (0, N)))

    def own_to(slot, d):
        for k in range(2):
            send(x_hbm, v_hbm, slot, k, d)

    @pl.when(first_chip == 1)
    def _():
        prepare()
        own_sum()

    with jax.named_scope("bar"):
        pl.semaphore_wait(bar, 2 - odd)
    pl.when(odd * (1 - c) == 1)(lambda: signal(note, partner))
    pl.when(last_chip == 1)(lambda: signal(peer, target))

    @pl.when(jnp.maximum(c, 1 - odd) == 1)
    def _():
        own_to(2 + 3 * dx, target)

    @pl.when(odd * c == 1)
    def _():
        pl.semaphore_wait(note, 1)

    own_to(4, partner)

    @pl.when(first_chip == 0)
    def _():
        prepare()

    @pl.when(odd * c == 1)
    def _():
        with jax.named_scope("peer"):
            pl.semaphore_wait(peer, 1)
        signal(note, partner)

    @pl.when(odd * (1 - c) == 1)
    def _():
        with jax.named_scope("go"):
            pl.semaphore_wait(note, 1)
        own_to(2 + 3 * dx, target)

    for k in range(2):
        arrive(4, k, "own4_")
        pass_on(4, 6 - 5 * dx, k, target)

    pl.when(first_chip == 0)(own_sum)
    tiles((4, team_of(0, 1), (0, N)))
    weight = jnp.sum(jnp.where(lax.broadcasted_iota(jnp.int32, (4, 4), 1) == t, mb[...].astype(jnp.float32), 0.0), axis=1, keepdims=True)

    f1, f2, p1, p2 = 5 - 3 * dx, 1 + 5 * dx, 6 - 5 * dx, 2 + 3 * dx

    def first(k):
        arrive(f1, k, "f1_")
        pass_on(f1, 1 + 5 * dx, k, partner)
        pass_on(f1, 7, k, target)
        return f1, team_of(1 - dx, 1 - dx), HALVES[k]

    def second(k):
        arrive(f2, k, "f2_")
        pass_on(f2, 5 - 3 * dx, k, partner)
        return f2, team_of(1 - dx, dx), HALVES[k]

    def third(k):
        arrive(7, k, "d7_")
        pass_on(7, 3, k, partner)
        return 7, team_of(1, 1), HALVES[k]

    def first_behind(k):
        arrive(p1, k, "p1_")
        return p1, team_of(dx, 1 - dx), HALVES[k]

    def second_behind(k):
        arrive(p2, k, "p2_")
        return p2, team_of(dx, dx), HALVES[k]

    def third_behind(k):
        arrive(3, k, "d3_")
        return 3, team_of(1, 0), HALVES[k]

    ahead = [(got, k) for got in (first, second, third) for k in range(2)]
    behind = [(got, k) for got in (first_behind, second_behind, third_behind) for k in range(2)]
    for g in range(7):
        group = ahead[g:g + 1] + (behind[g - 1:g] if g else [])
        tiles(*[got(k) for got, k in group])

    o_ref[...] = jnp.sum(fb[0:4] * weight, axis=0, keepdims=True)
    with jax.named_scope("sendw"):
        copy_x(xb.at[0:7], xb.at[1:8], 1, 0, partner).wait_send()
        copy = pltpu.make_async_remote_copy(src_ref=vb.at[0:7], dst_ref=vb.at[1:8], send_sem=sent_v, recv_sem=got_v.at[0], device_id=partner, device_id_type=MESH)
        copy.wait_send()


SEMS = [
    pltpu.SemaphoreType.DMA((3,)),
    pltpu.SemaphoreType.DMA,
    pltpu.SemaphoreType.DMA,
    pltpu.SemaphoreType.DMA((7, 2)),
    pltpu.SemaphoreType.DMA((7,)),
    pltpu.SemaphoreType.REGULAR,
    pltpu.SemaphoreType.REGULAR,
]


def kernel(*refs):
    if SCOPED:
        pl.run_scoped(functools.partial(body, *refs), *SEMS)
    else:
        body(*refs)


def solution(mesh):
    spec = P(("dp", "team", "rep"), None)

    def per_device(points, values, pair_mask, bandwidth):
        hbm = [pltpu.with_memory_space_constraint(z, pltpu.HBM) for z in (points.T, values.T, pair_mask)]
        field = pl.pallas_call(
            kernel,
            out_shape=jax.ShapeDtypeStruct((1, N), jnp.float32),
            in_specs=[pl.BlockSpec(memory_space=pltpu.HBM)] * 3 + [pl.BlockSpec(memory_space=pltpu.SMEM)],
            out_specs=pl.BlockSpec(memory_space=pltpu.VMEM),
            scratch_shapes=[
                pltpu.VMEM((8, 90, N), jnp.bfloat16),
                pltpu.VMEM((8, 1, N), jnp.bfloat16),
                pltpu.VMEM((4, 4), jnp.int32),
                pltpu.VMEM((96, N), jnp.bfloat16),
                pltpu.VMEM((16, N), jnp.float32),
                *(() if SCOPED else SEMS),
            ],
            compiler_params=pltpu.CompilerParams(collective_id=0, has_side_effects=True, vmem_limit_bytes=16 * 2**20),
        )(*hbm, bandwidth)
        return field.T

    return jax.shard_map(per_device, mesh=mesh, in_specs=(spec, spec, P("dp", None), P()), out_specs=spec, check_vma=False)
```

```python
import functools

import jax
import jax.numpy as jnp
from jax import lax
from jax.experimental import pallas as pl
from jax.experimental.pallas import tpu as pltpu
from jax.sharding import PartitionSpec as P

MESH = pl.DeviceIdType.MESH
N = 1024
LOG2E = 1.4426950408889634
TJ = 256
TI = 512
LAG = 3
SCOPED = 1
LTJ = 512
LTI = 512
LLAG = 1
NOCOMP = 0
HALVES = ((0, 512), (512, 512))


def split3(s):
    hi = s.astype(jnp.bfloat16).astype(jnp.float32)
    rest = s - hi
    mid = rest.astype(jnp.bfloat16).astype(jnp.float32)
    return hi, mid, rest - mid


def augment(xt, rest, weights):
    n = xt.shape[1]
    x32 = xt.astype(jnp.float32)
    r32 = rest.astype(jnp.float32)
    hi, mid, lo = split3(jnp.sum(x32 * x32, axis=0, keepdims=True) + jnp.sum(r32 * r32, axis=0, keepdims=True))
    last = jnp.concatenate([x32[80:88], r32, jnp.zeros((6, n), jnp.float32)], axis=0)
    row = lax.broadcasted_iota(jnp.int32, (16, n), 0)
    if weights:
        tail = jnp.where(row < 10, -2.0 * last, jnp.where(row < 13, 1.0, jnp.where(row == 13, hi, jnp.where(row == 14, mid, lo))))
        return jnp.concatenate([(-2.0 * x32[:80]).astype(jnp.bfloat16), tail.astype(jnp.bfloat16)], axis=0)
    tail = jnp.where(row < 10, last, jnp.where(row >= 13, 1.0, jnp.where(row == 10, hi, jnp.where(row == 11, mid, lo))))
    return jnp.concatenate([xt[:80], tail.astype(jnp.bfloat16)], axis=0)


def body(x_hbm, v_hbm, m_hbm, h_ref, o_ref, xb, rb, vb, mb, wb, fb, load_sem, sent_x, sent_r, sent_v, got_x, got_r, got_v, note, peer):
    y, t, dp = lax.axis_index("rep"), lax.axis_index("team"), lax.axis_index("dp")
    x, c = t // 2, t % 2
    dx = c + y - 2 * c * y
    odd = x + y - 2 * x * y
    first_chip, last_chip = (1 - x) * (1 - y), x * y

    def dev(fx, fy, fc):
        return (dp, y + fy - 2 * y * fy, 2 * (x + fx - 2 * x * fx) + c + fc - 2 * c * fc)

    def team_of(fx, fc):
        return 2 * (x + fx - 2 * x * fx) + c + fc - 2 * c * fc

    partner, target, source = dev(0, 0, 1), dev(dx, 1 - dx, dx), dev(1 - dx, dx, 1 - dx)

    def signal(sem, d):
        pl.semaphore_signal(sem, inc=1, device_id=d, device_id_type=MESH)

    bar = pltpu.get_barrier_semaphore()
    pl.when(last_chip == 0)(lambda: signal(bar, source))
    pl.when(jnp.maximum(c, 1 - odd) == 1)(lambda: signal(bar, partner))
    loads = [pltpu.make_async_copy(src, dst, load_sem.at[i]) for i, (src, dst) in enumerate(((x_hbm.at[0:88], xb.at[0]), (x_hbm.at[88:90], rb.at[0]), (v_hbm, vb.at[0]), (m_hbm, mb)))]
    for z in loads:
        z.start()
    def copy_x(src, dst, slot, k, d):
        return pltpu.make_async_remote_copy(src_ref=src, dst_ref=dst, send_sem=sent_x, recv_sem=got_x.at[slot - 1, k], device_id=d, device_id_type=MESH)

    def copy_v(src, slot, d):
        return pltpu.make_async_remote_copy(src_ref=src, dst_ref=vb.at[slot], send_sem=sent_v, recv_sem=got_v.at[slot - 1], device_id=d, device_id_type=MESH)

    def copy_r(src, slot, d):
        return pltpu.make_async_remote_copy(src_ref=src, dst_ref=rb.at[slot], send_sem=sent_r, recv_sem=got_r.at[slot - 1], device_id=d, device_id_type=MESH)

    def send(x_src, r_src, v_src, slot, k, d):
        cols = pl.ds(*HALVES[k])
        if k == 0:
            copy_r(r_src, slot, d).start()
        copy_x(x_src.at[:, cols], xb.at[slot, :, cols], slot, k, d).start()
        if k == 0:
            copy_v(v_src, slot, d).start()

    def pass_on(slot, to, k, d):
        send(xb.at[slot], rb.at[slot], vb.at[slot], to, k, d)

    def arrive(slot, k, name):
        with jax.named_scope(f"{name}{k}"):
            if k == 0:
                copy_v(vb.at[slot], slot, partner).wait_recv()
                copy_r(rb.at[slot], slot, partner).wait_recv()
            ref = xb.at[slot, :, pl.ds(*HALVES[k])]
            copy_x(ref, ref, slot, k, partner).wait_recv()

    alpha = -LOG2E / h_ref[0]

    def tiles(*parts, tj=TJ, ti=TI, lag=LAG):
        if NOCOMP:
            return
        total, pend = {}, []

        def drain():
            i, vv, d = pend.pop(0)
            kern = jnp.exp2(d * alpha).astype(jnp.bfloat16)
            r = jnp.dot(vv, kern, preferred_element_type=jnp.float32)
            total[i] = total[i] + r if i in total else r

        with jax.named_scope("tiles"):
            for slot, team, at in parts:
                lhs = augment(xb[slot, :, at[0]:at[0] + at[1]], rb[slot, :, at[0]:at[0] + at[1]], False).T
                for j in range(0, at[1], tj):
                    rows = lax.broadcasted_iota(jnp.int32, (16, tj), 0)
                    v32 = vb[slot, :, at[0] + j:at[0] + j + tj].astype(jnp.float32)
                    vv = jnp.where(rows == team, jnp.broadcast_to(v32, (16, tj)), 0.0).astype(jnp.bfloat16)
                    for i in range(0, N, ti):
                        pend.append((i, vv, jnp.dot(lhs[j:j + tj], wb[:, i:i + ti], preferred_element_type=jnp.float32)))
                        if len(pend) > lag:
                            drain()
            while pend:
                drain()
            for i in total:
                fb[:, i:i + ti] += total[i]

    def prepare():
        fb[...] = jnp.zeros_like(fb)
        for z in loads:
            z.wait()
        for i in range(0, N, 256):
            wb[:, i:i + 256] = augment(xb[0, :, i:i + 256], rb[0, :, i:i + 256], True)

    def own_sum():
        tiles((0, team_of(0, 0), (0, N)))

    def own_to(slot, d):
        for k in range(2):
            send(x_hbm.at[0:88], x_hbm.at[88:90], v_hbm, slot, k, d)

    @pl.when(first_chip == 1)
    def _():
        prepare()
        own_sum()

    with jax.named_scope("bar"):
        pl.semaphore_wait(bar, 2 - odd)
    pl.when(odd * (1 - c) == 1)(lambda: signal(note, partner))
    pl.when(last_chip == 1)(lambda: signal(peer, target))

    @pl.when(jnp.maximum(c, 1 - odd) == 1)
    def _():
        own_to(2 + 3 * dx, target)

    @pl.when(odd * c == 1)
    def _():
        pl.semaphore_wait(note, 1)

    own_to(4, partner)

    @pl.when(first_chip == 0)
    def _():
        prepare()

    @pl.when(odd * c == 1)
    def _():
        with jax.named_scope("peer"):
            pl.semaphore_wait(peer, 1)
        signal(note, partner)

    @pl.when(odd * (1 - c) == 1)
    def _():
        with jax.named_scope("go"):
            pl.semaphore_wait(note, 1)
        own_to(2 + 3 * dx, target)

    for k in range(2):
        arrive(4, k, "own4_")
        pass_on(4, 6 - 5 * dx, k, target)

    pl.when(first_chip == 0)(own_sum)
    tiles((4, team_of(0, 1), (0, N)))
    weight = jnp.sum(jnp.where(lax.broadcasted_iota(jnp.int32, (4, 4), 1) == t, mb[...].astype(jnp.float32), 0.0), axis=1, keepdims=True)

    f1, f2, p1, p2 = 5 - 3 * dx, 1 + 5 * dx, 6 - 5 * dx, 2 + 3 * dx

    def first(k):
        arrive(f1, k, "f1_")
        pass_on(f1, 1 + 5 * dx, k, partner)
        pass_on(f1, 7, k, target)
        return f1, team_of(1 - dx, 1 - dx), HALVES[k]

    def second(k):
        arrive(f2, k, "f2_")
        pass_on(f2, 5 - 3 * dx, k, partner)
        return f2, team_of(1 - dx, dx), HALVES[k]

    def third(k):
        arrive(7, k, "d7_")
        pass_on(7, 3, k, partner)
        return 7, team_of(1, 1), HALVES[k]

    def first_behind(k):
        arrive(p1, k, "p1_")
        return p1, team_of(dx, 1 - dx), HALVES[k]

    def second_behind(k):
        arrive(p2, k, "p2_")
        return p2, team_of(dx, dx), HALVES[k]

    def third_behind(k):
        arrive(3, k, "d3_")
        return 3, team_of(1, 0), HALVES[k]

    ahead = [(got, k) for got in (first, second, third) for k in range(2)]
    behind = [(got, k) for got in (first_behind, second_behind, third_behind) for k in range(2)]
    for g in range(7):
        group = ahead[g:g + 1] + (behind[g - 1:g] if g else [])
        parts = [got(k) for got, k in group]
        if g < 6:
            tiles(*parts)
        else:
            tiles(*parts, tj=LTJ, ti=LTI, lag=LLAG)

    o_ref[...] = jnp.sum(fb[0:4] * weight, axis=0, keepdims=True)
    with jax.named_scope("sendw"):
        copy_x(xb.at[0:7], xb.at[1:8], 1, 0, partner).wait_send()
        pltpu.make_async_remote_copy(src_ref=rb.at[0:7], dst_ref=rb.at[1:8], send_sem=sent_r, recv_sem=got_r.at[0], device_id=partner, device_id_type=MESH).wait_send()
        copy = pltpu.make_async_remote_copy(src_ref=vb.at[0:7], dst_ref=vb.at[1:8], send_sem=sent_v, recv_sem=got_v.at[0], device_id=partner, device_id_type=MESH)
        copy.wait_send()


SEMS = [
    pltpu.SemaphoreType.DMA((4,)),
    pltpu.SemaphoreType.DMA,
    pltpu.SemaphoreType.DMA,
    pltpu.SemaphoreType.DMA,
    pltpu.SemaphoreType.DMA((7, 2)),
    pltpu.SemaphoreType.DMA((7,)),
    pltpu.SemaphoreType.DMA((7,)),
    pltpu.SemaphoreType.REGULAR,
    pltpu.SemaphoreType.REGULAR,
]


def kernel(*refs):
    if SCOPED:
        pl.run_scoped(functools.partial(body, *refs), *SEMS)
    else:
        body(*refs)


def solution(mesh):
    spec = P(("dp", "team", "rep"), None)

    def per_device(points, values, pair_mask, bandwidth):
        hbm = [pltpu.with_memory_space_constraint(z, pltpu.HBM) for z in (points.T, values.T, pair_mask)]
        field = pl.pallas_call(
            kernel,
            out_shape=jax.ShapeDtypeStruct((1, N), jnp.float32),
            in_specs=[pl.BlockSpec(memory_space=pltpu.HBM)] * 3 + [pl.BlockSpec(memory_space=pltpu.SMEM)],
            out_specs=pl.BlockSpec(memory_space=pltpu.VMEM),
            scratch_shapes=[
                pltpu.VMEM((8, 88, N), jnp.bfloat16),
                pltpu.VMEM((8, 2, N), jnp.bfloat16),
                pltpu.VMEM((8, 1, N), jnp.bfloat16),
                pltpu.VMEM((4, 4), jnp.int32),
                pltpu.VMEM((96, N), jnp.bfloat16),
                pltpu.VMEM((16, N), jnp.float32),
                *(() if SCOPED else SEMS),
            ],
            compiler_params=pltpu.CompilerParams(collective_id=0, has_side_effects=True, vmem_limit_bytes=16 * 2**20),
        )(*hbm, bandwidth)
        return field.T

    return jax.shard_map(per_device, mesh=mesh, in_specs=(spec, spec, P("dp", None), P()), out_specs=spec, check_vma=False)
```

```python
import functools

import jax
import jax.numpy as jnp
from jax import lax
from jax.experimental import pallas as pl
from jax.experimental.pallas import tpu as pltpu
from jax.sharding import PartitionSpec as P

MESH = pl.DeviceIdType.MESH
N = 1024
LOG2E = 1.4426950408889634
WIDE = 2.0**64
TJ, TI, LAG = 512, 512, 1
HALVES = ((0, 512), (512, 512))


def split3(s):
    hi = s.astype(jnp.bfloat16).astype(jnp.float32)
    rest = s - hi
    mid = rest.astype(jnp.bfloat16).astype(jnp.float32)
    return hi, mid, rest - mid


def augment(xt, rest, scale=None):
    n = xt.shape[1]
    x32 = xt.astype(jnp.float32)
    r32 = rest.astype(jnp.float32)
    hi, mid, lo = split3(jnp.sum(x32 * x32, axis=0, keepdims=True) + jnp.sum(r32 * r32, axis=0, keepdims=True))
    last = jnp.concatenate([x32[80:88], r32, jnp.zeros((6, n), jnp.float32)], axis=0)
    row = lax.broadcasted_iota(jnp.int32, (16, n), 0)
    if scale is not None:
        tail = jnp.where(row < 10, -2.0 * last, jnp.where(row < 13, 1.0, jnp.where(row == 13, hi, jnp.where(row == 14, mid, lo))))
        return jnp.concatenate([(-2.0 * scale * x32[:80]).astype(jnp.bfloat16), (scale * tail).astype(jnp.bfloat16)], axis=0)
    tail = jnp.where(row < 10, last, jnp.where(row >= 13, 1.0, jnp.where(row == 10, hi, jnp.where(row == 11, mid, lo))))
    return jnp.concatenate([xt[:80], tail.astype(jnp.bfloat16)], axis=0)


def body(x_hbm, v_hbm, m_hbm, h_ref, o_ref, xb, rb, vb, mb, wb, fb, load_sem, sent_x, sent_r, sent_v, got_x, got_r, got_v, note, peer):
    y, t, dp = lax.axis_index("rep"), lax.axis_index("team"), lax.axis_index("dp")
    x, c = t // 2, t % 2
    dx = c + y - 2 * c * y
    odd = x + y - 2 * x * y
    first_chip, last_chip = (1 - x) * (1 - y), x * y

    def dev(fx, fy, fc):
        return (dp, y + fy - 2 * y * fy, 2 * (x + fx - 2 * x * fx) + c + fc - 2 * c * fc)

    def team_of(fx, fc):
        return 2 * (x + fx - 2 * x * fx) + c + fc - 2 * c * fc

    partner, target, source = dev(0, 0, 1), dev(dx, 1 - dx, dx), dev(1 - dx, dx, 1 - dx)

    def signal(sem, d):
        pl.semaphore_signal(sem, inc=1, device_id=d, device_id_type=MESH)

    bar = pltpu.get_barrier_semaphore()
    pl.when(last_chip == 0)(lambda: signal(bar, source))
    pl.when(jnp.maximum(c, 1 - odd) == 1)(lambda: signal(bar, partner))
    loads = [pltpu.make_async_copy(src, dst, load_sem.at[i]) for i, (src, dst) in enumerate(((x_hbm.at[0:88], xb.at[0]), (x_hbm.at[88:90], rb.at[0]), (v_hbm, vb.at[0]), (m_hbm, mb)))]

    def load():
        for z in loads:
            z.start()

    pl.when(first_chip == 1)(load)

    def copy_x(src, dst, slot, k, d):
        return pltpu.make_async_remote_copy(src_ref=src, dst_ref=dst, send_sem=sent_x, recv_sem=got_x.at[slot - 1, k], device_id=d, device_id_type=MESH)

    def copy_v(src, slot, d):
        return pltpu.make_async_remote_copy(src_ref=src, dst_ref=vb.at[slot], send_sem=sent_v, recv_sem=got_v.at[slot - 1], device_id=d, device_id_type=MESH)

    def copy_r(src, slot, d):
        return pltpu.make_async_remote_copy(src_ref=src, dst_ref=rb.at[slot], send_sem=sent_r, recv_sem=got_r.at[slot - 1], device_id=d, device_id_type=MESH)

    def send(x_src, r_src, v_src, slot, k, d):
        cols = pl.ds(*HALVES[k])
        if k == 0:
            copy_r(r_src, slot, d).start()
        copy_x(x_src.at[:, cols], xb.at[slot, :, cols], slot, k, d).start()
        if k == 0:
            copy_v(v_src, slot, d).start()

    def pass_on(slot, to, k, d):
        send(xb.at[slot], rb.at[slot], vb.at[slot], to, k, d)

    def arrive(slot, k, name):
        with jax.named_scope(f"{name}{k}"):
            if k == 0:
                copy_v(vb.at[slot], slot, partner).wait_recv()
                copy_r(rb.at[slot], slot, partner).wait_recv()
            ref = xb.at[slot, :, pl.ds(*HALVES[k])]
            copy_x(ref, ref, slot, k, partner).wait_recv()

    scale = jnp.where(h_ref[0] > WIDE, 1.0 / WIDE, 1.0)
    alpha = -LOG2E / (h_ref[0] * scale)

    def tiles(*parts):
        total, pend = {}, []

        def drain():
            i, vv, d = pend.pop(0)
            kern = jnp.exp2(d * alpha).astype(jnp.bfloat16)
            r = jnp.dot(vv, kern, preferred_element_type=jnp.float32)
            total[i] = total[i] + r if i in total else r

        with jax.named_scope("tiles"):
            for slot, team, at in parts:
                lhs = augment(xb[slot, :, at[0]:at[0] + at[1]], rb[slot, :, at[0]:at[0] + at[1]]).T
                for j in range(0, at[1], TJ):
                    rows = lax.broadcasted_iota(jnp.int32, (16, TJ), 0)
                    v32 = vb[slot, :, at[0] + j:at[0] + j + TJ].astype(jnp.float32)
                    vv = jnp.where(rows == team, jnp.broadcast_to(v32, (16, TJ)), 0.0).astype(jnp.bfloat16)
                    for i in range(0, N, TI):
                        pend.append((i, vv, jnp.dot(lhs[j:j + TJ], wb[:, i:i + TI], preferred_element_type=jnp.float32)))
                        if len(pend) > LAG:
                            drain()
            while pend:
                drain()
            for i in total:
                fb[:, i:i + TI] += total[i]

    def prepare():
        fb[...] = jnp.zeros_like(fb)
        for z in loads:
            z.wait()
        for i in range(0, N, 256):
            wb[:, i:i + 256] = augment(xb[0, :, i:i + 256], rb[0, :, i:i + 256], scale)

    def own_sum():
        tiles((0, team_of(0, 0), (0, N)))

    def own_to(slot, d):
        for k in range(2):
            send(x_hbm.at[0:88], x_hbm.at[88:90], v_hbm, slot, k, d)

    @pl.when(first_chip == 1)
    def _():
        prepare()
        own_sum()

    with jax.named_scope("bar"):
        pl.semaphore_wait(bar, 2 - odd)
    @pl.when(jnp.maximum(c, 1 - odd) == 1)
    def _():
        own_to(2 + 3 * dx, target)

    pl.when(last_chip == 1)(lambda: signal(peer, target))
    pl.when(odd * (1 - c) == 1)(lambda: signal(note, partner))
    pl.when(first_chip == 0)(load)

    @pl.when(odd * c == 1)
    def _():
        pl.semaphore_wait(note, 1)

    own_to(4, partner)

    @pl.when(first_chip == 0)
    def _():
        prepare()

    @pl.when(odd * c == 1)
    def _():
        with jax.named_scope("peer"):
            pl.semaphore_wait(peer, 1)
        signal(note, partner)

    @pl.when(odd * (1 - c) == 1)
    def _():
        with jax.named_scope("go"):
            pl.semaphore_wait(note, 1)
        own_to(2 + 3 * dx, target)

    for k in range(2):
        arrive(4, k, "own4_")
        pass_on(4, 6 - 5 * dx, k, target)

    pl.when(first_chip == 0)(own_sum)
    tiles((4, team_of(0, 1), (0, N)))
    weight = jnp.sum(jnp.where(lax.broadcasted_iota(jnp.int32, (4, 4), 1) == t, mb[...].astype(jnp.float32), 0.0), axis=1, keepdims=True)

    f1, f2, p1, p2 = 5 - 3 * dx, 1 + 5 * dx, 6 - 5 * dx, 2 + 3 * dx

    def first(k):
        arrive(f1, k, "f1_")
        pass_on(f1, 1 + 5 * dx, k, partner)
        pass_on(f1, 7, k, target)
        return f1, team_of(1 - dx, 1 - dx), HALVES[k]

    def second(k):
        arrive(f2, k, "f2_")
        pass_on(f2, 5 - 3 * dx, k, partner)
        return f2, team_of(1 - dx, dx), HALVES[k]

    def third(k):
        arrive(7, k, "d7_")
        pass_on(7, 3, k, partner)
        return 7, team_of(1, 1), HALVES[k]

    def first_behind(k):
        arrive(p1, k, "p1_")
        return p1, team_of(dx, 1 - dx), HALVES[k]

    def second_behind(k):
        arrive(p2, k, "p2_")
        return p2, team_of(dx, dx), HALVES[k]

    def third_behind(k):
        arrive(3, k, "d3_")
        return 3, team_of(1, 0), HALVES[k]

    ahead = [(got, k) for got in (first, second, third) for k in range(2)]
    behind = [(got, k) for got in (first_behind, second_behind, third_behind) for k in range(2)]
    for g in range(7):
        group = ahead[g:g + 1] + (behind[g - 1:g] if g else [])
        tiles(*[got(k) for got, k in group])

    o_ref[...] = jnp.sum(fb[0:4] * weight, axis=0, keepdims=True)
    with jax.named_scope("sendw"):
        copy_x(xb.at[0:7], xb.at[1:8], 1, 0, partner).wait_send()
        pltpu.make_async_remote_copy(src_ref=rb.at[0:7], dst_ref=rb.at[1:8], send_sem=sent_r, recv_sem=got_r.at[0], device_id=partner, device_id_type=MESH).wait_send()
        copy = pltpu.make_async_remote_copy(src_ref=vb.at[0:7], dst_ref=vb.at[1:8], send_sem=sent_v, recv_sem=got_v.at[0], device_id=partner, device_id_type=MESH)
        copy.wait_send()


SEMS = [
    pltpu.SemaphoreType.DMA((4,)),
    pltpu.SemaphoreType.DMA,
    pltpu.SemaphoreType.DMA,
    pltpu.SemaphoreType.DMA,
    pltpu.SemaphoreType.DMA((7, 2)),
    pltpu.SemaphoreType.DMA((7,)),
    pltpu.SemaphoreType.DMA((7,)),
    pltpu.SemaphoreType.REGULAR,
    pltpu.SemaphoreType.REGULAR,
]


def kernel(*refs):
    pl.run_scoped(functools.partial(body, *refs), *SEMS)


def solution(mesh):
    spec = P(("dp", "team", "rep"), None)

    def per_device(points, values, pair_mask, bandwidth):
        hbm = [pltpu.with_memory_space_constraint(z, pltpu.HBM) for z in (points.T, values.T, pair_mask)]
        field = pl.pallas_call(
            kernel,
            out_shape=jax.ShapeDtypeStruct((1, N), jnp.float32),
            in_specs=[pl.BlockSpec(memory_space=pltpu.HBM)] * 3 + [pl.BlockSpec(memory_space=pltpu.SMEM)],
            out_specs=pl.BlockSpec(memory_space=pltpu.VMEM),
            scratch_shapes=[
                pltpu.VMEM((8, 88, N), jnp.bfloat16),
                pltpu.VMEM((8, 2, N), jnp.bfloat16),
                pltpu.VMEM((8, 1, N), jnp.bfloat16),
                pltpu.VMEM((4, 4), jnp.int32),
                pltpu.VMEM((96, N), jnp.bfloat16),
                pltpu.VMEM((16, N), jnp.float32),
            ],
            compiler_params=pltpu.CompilerParams(collective_id=0, has_side_effects=True, vmem_limit_bytes=16 * 2**20),
        )(*hbm, bandwidth)
        return field.T

    return jax.shard_map(per_device, mesh=mesh, in_specs=(spec, spec, P("dp", None), P()), out_specs=spec, check_vma=False)
```

```python
import functools

import jax
import jax.numpy as jnp
from jax import lax
from jax.experimental import pallas as pl
from jax.experimental.pallas import tpu as pltpu
from jax.sharding import PartitionSpec as P

MESH = pl.DeviceIdType.MESH
N = 1024
LOG2E = 1.4426950408889634
WIDE = 2.0**64
TJ, TI, LAG = 512, 512, 1
HALVES = ((0, 512), (512, 512))
KEPT = 256


def split3(s):
    hi = s.astype(jnp.bfloat16).astype(jnp.float32)
    rest = s - hi
    mid = rest.astype(jnp.bfloat16).astype(jnp.float32)
    return hi, mid, rest - mid


def augment(xt, rest, scale=None):
    n = xt.shape[1]
    x32 = xt.astype(jnp.float32)
    r32 = rest.astype(jnp.float32)
    hi, mid, lo = split3(jnp.sum(x32 * x32, axis=0, keepdims=True) + jnp.sum(r32 * r32, axis=0, keepdims=True))
    last = jnp.concatenate([x32[80:88], r32, jnp.zeros((6, n), jnp.float32)], axis=0)
    row = lax.broadcasted_iota(jnp.int32, (16, n), 0)
    if scale is not None:
        tail = jnp.where(row < 10, -2.0 * last, jnp.where(row < 13, 1.0, jnp.where(row == 13, hi, jnp.where(row == 14, mid, lo))))
        return jnp.concatenate([(-2.0 * scale * x32[:80]).astype(jnp.bfloat16), (scale * tail).astype(jnp.bfloat16)], axis=0)
    tail = jnp.where(row < 10, last, jnp.where(row >= 13, 1.0, jnp.where(row == 10, hi, jnp.where(row == 11, mid, lo))))
    return jnp.concatenate([xt[:80], tail.astype(jnp.bfloat16)], axis=0)


def body(x_hbm, v_hbm, m_hbm, h_ref, o_ref, xb, rb, vb, mb, wb, fb, wp, fp, part_out, part_in, load_sem, sent_x, sent_r, sent_v, sent_t, sent_p, got_x, got_r, got_v, got_p, note, peer):
    y, t, dp = lax.axis_index("rep"), lax.axis_index("team"), lax.axis_index("dp")
    x, c = t // 2, t % 2
    dx = c + y - 2 * c * y
    odd = x + y - 2 * x * y
    first_chip, last_chip = (1 - x) * (1 - y), x * y

    def dev(fx, fy, fc):
        return (dp, y + fy - 2 * y * fy, 2 * (x + fx - 2 * x * fx) + c + fc - 2 * c * fc)

    def team_of(fx, fc):
        return 2 * (x + fx - 2 * x * fx) + c + fc - 2 * c * fc

    partner, target, source = dev(0, 0, 1), dev(dx, 1 - dx, dx), dev(1 - dx, dx, 1 - dx)

    def signal(sem, d):
        pl.semaphore_signal(sem, inc=1, device_id=d, device_id_type=MESH)

    bar = pltpu.get_barrier_semaphore()
    pl.when(last_chip == 0)(lambda: signal(bar, source))
    pl.when(jnp.maximum(c, 1 - odd) == 1)(lambda: signal(bar, partner))
    loads = [pltpu.make_async_copy(src, dst, load_sem.at[i]) for i, (src, dst) in enumerate(((x_hbm.at[0:88], xb.at[0]), (x_hbm.at[88:90], rb.at[0]), (v_hbm, vb.at[0]), (m_hbm, mb)))]

    def load():
        for z in loads:
            z.start()

    pl.when(first_chip == 1)(load)

    def copy_x(src, dst, slot, k, d, sent=sent_x):
        return pltpu.make_async_remote_copy(src_ref=src, dst_ref=dst, send_sem=sent, recv_sem=got_x.at[slot - 1, k], device_id=d, device_id_type=MESH)

    def copy_v(src, slot, d):
        return pltpu.make_async_remote_copy(src_ref=src, dst_ref=vb.at[slot], send_sem=sent_v, recv_sem=got_v.at[slot - 1], device_id=d, device_id_type=MESH)

    def copy_r(src, slot, d):
        return pltpu.make_async_remote_copy(src_ref=src, dst_ref=rb.at[slot], send_sem=sent_r, recv_sem=got_r.at[slot - 1], device_id=d, device_id_type=MESH)

    def send(x_src, r_src, v_src, slot, k, d, at=None, sent=sent_x):
        cols = pl.ds(*(at or HALVES[k]))
        if k == 0:
            copy_r(r_src, slot, d).start()
        copy_x(x_src.at[:, cols], xb.at[slot, :, cols], slot, k, d, sent).start()
        if k == 0:
            copy_v(v_src, slot, d).start()

    def pass_on(slot, to, k, d, at=None, sent=sent_x):
        send(xb.at[slot], rb.at[slot], vb.at[slot], to, k, d, at, sent)

    def arrive(slot, k, name, at=None):
        with jax.named_scope(f"{name}{k}"):
            if k == 0:
                copy_v(vb.at[slot], slot, partner).wait_recv()
                copy_r(rb.at[slot], slot, partner).wait_recv()
            ref = xb.at[slot, :, pl.ds(*(at or HALVES[k]))]
            copy_x(ref, ref, slot, k, partner).wait_recv()

    scale = jnp.where(h_ref[0] > WIDE, 1.0 / WIDE, 1.0)
    alpha = -LOG2E / (h_ref[0] * scale)

    def tiles(*parts, weights=wb, sums=fb):
        total, pend = {}, []

        def drain():
            i, vv, d = pend.pop(0)
            kern = jnp.exp2(d * alpha).astype(jnp.bfloat16)
            r = jnp.dot(vv, kern, preferred_element_type=jnp.float32)
            total[i] = total[i] + r if i in total else r

        with jax.named_scope("tiles"):
            for slot, team, at in parts:
                lhs = augment(xb[slot, :, at[0]:at[0] + at[1]], rb[slot, :, at[0]:at[0] + at[1]]).T
                for j in range(0, at[1], TJ):
                    size = min(TJ, at[1] - j)
                    rows = lax.broadcasted_iota(jnp.int32, (16, size), 0)
                    v32 = vb[slot, :, at[0] + j:at[0] + j + size].astype(jnp.float32)
                    vv = jnp.where(rows == team, jnp.broadcast_to(v32, (16, size)), 0.0).astype(jnp.bfloat16)
                    for i in range(0, N, TI):
                        pend.append((i, vv, jnp.dot(lhs[j:j + size], weights[:, i:i + TI], preferred_element_type=jnp.float32)))
                        if len(pend) > LAG:
                            drain()
            while pend:
                drain()
            for i in total:
                sums[:, i:i + TI] += total[i]

    def prepare():
        fb[...] = jnp.zeros_like(fb)
        for z in loads:
            z.wait()
        for i in range(0, N, 256):
            wb[:, i:i + 256] = augment(xb[0, :, i:i + 256], rb[0, :, i:i + 256], scale)

    def own_sum():
        tiles((0, team_of(0, 0), (0, N)))

    def own_to(slot, d):
        for k in range(2):
            send(x_hbm.at[0:88], x_hbm.at[88:90], v_hbm, slot, k, d)

    @pl.when(first_chip == 1)
    def _():
        prepare()
        own_sum()

    with jax.named_scope("bar"):
        pl.semaphore_wait(bar, 2 - odd)
    @pl.when(jnp.maximum(c, 1 - odd) == 1)
    def _():
        own_to(2 + 3 * dx, target)

    pl.when(last_chip == 1)(lambda: signal(peer, target))
    pl.when(odd * (1 - c) == 1)(lambda: signal(note, partner))
    pl.when(first_chip == 0)(load)

    @pl.when(odd * c == 1)
    def _():
        pl.semaphore_wait(note, 1)

    own_to(4, partner)

    @pl.when(first_chip == 0)
    def _():
        prepare()

    @pl.when(odd * c == 1)
    def _():
        with jax.named_scope("peer"):
            pl.semaphore_wait(peer, 1)
        signal(note, partner)

    @pl.when(odd * (1 - c) == 1)
    def _():
        with jax.named_scope("go"):
            pl.semaphore_wait(note, 1)
        own_to(2 + 3 * dx, target)

    for k in range(2):
        arrive(4, k, "own4_")
        pass_on(4, 6 - 5 * dx, k, target)

    pl.when(first_chip == 0)(own_sum)
    tiles((4, team_of(0, 1), (0, N)))
    def weight_of(team):
        mine = lax.broadcasted_iota(jnp.int32, (4, 4), 1) == team
        return jnp.sum(jnp.where(mine, mb[...].astype(jnp.float32), 0.0), axis=1, keepdims=True)

    weight = weight_of(t)

    @pl.when(dx == 1)
    def _():
        fp[...] = jnp.zeros_like(fp)
        for i in range(0, N, 256):
            wp[:, i:i + 256] = augment(xb[4, :, i:i + 256], rb[4, :, i:i + 256], scale)


    f1, f2, p1, p2 = 5 - 3 * dx, 1 + 5 * dx, 6 - 5 * dx, 2 + 3 * dx

    def first(k):
        arrive(f1, k, "f1_")
        pass_on(f1, 1 + 5 * dx, k, partner)
        pass_on(f1, 7, k, target)
        return f1, team_of(1 - dx, 1 - dx), HALVES[k]

    def second(k):
        arrive(f2, k, "f2_")
        pass_on(f2, 5 - 3 * dx, k, partner)
        return f2, team_of(1 - dx, dx), HALVES[k]

    def first_behind(k):
        arrive(p1, k, "p1_")
        return p1, team_of(dx, 1 - dx), HALVES[k]

    def second_behind(k):
        arrive(p2, k, "p2_")
        return p2, team_of(dx, dx), HALVES[k]

    direct, behind = (7, team_of(1, 1)), (3, team_of(1, 0))
    cut = (HALVES[1][0], HALVES[1][1] - KEPT)
    kept = (N - KEPT, KEPT)
    partial = pltpu.make_async_remote_copy(src_ref=part_out, dst_ref=part_in, send_sem=sent_p, recv_sem=got_p, device_id=partner, device_id_type=MESH)

    def third(k, at=None):
        arrive(7, k, "d7_")
        pass_on(7, 3, k, partner, at, sent_t)

    tiles(first(0))
    tiles(first(1), first_behind(0))
    tiles(second(0), first_behind(1))
    tiles(second(1), second_behind(0))
    third(0)
    tiles((*direct, HALVES[0]), second_behind(1))

    @pl.when(dx == 0)
    def _():
        third(1)
        arrive(3, 0, "d3_")
        tiles((*direct, HALVES[1]), (*behind, HALVES[0]))
        arrive(3, 1, "d3_", cut)
        tiles((*behind, cut))
        partial.wait_recv()
        o_ref[...] = jnp.sum(fb[0:4] * weight, axis=0, keepdims=True) + part_in[...]

    @pl.when(dx == 1)
    def _():
        third(1, cut)
        tiles((*direct, kept), weights=wp, sums=fp)
        part_out[...] = jnp.sum(fp[0:4] * weight_of(team_of(0, 1)), axis=0, keepdims=True)
        arrive(3, 0, "d3_")
        partial.start()
        tiles((*direct, HALVES[1]), (*behind, HALVES[0]))
        arrive(3, 1, "d3_")
        tiles((*behind, HALVES[1]))
        o_ref[...] = jnp.sum(fb[0:4] * weight, axis=0, keepdims=True)

    with jax.named_scope("sendw"):
        copy_x(xb.at[0:6], xb.at[1:7], 1, 0, partner).wait_send()
        pltpu.make_async_remote_copy(src_ref=rb.at[0:7], dst_ref=rb.at[1:8], send_sem=sent_r, recv_sem=got_r.at[0], device_id=partner, device_id_type=MESH).wait_send()
        copy = pltpu.make_async_remote_copy(src_ref=vb.at[0:7], dst_ref=vb.at[1:8], send_sem=sent_v, recv_sem=got_v.at[0], device_id=partner, device_id_type=MESH)
        copy.wait_send()

        @pl.when(dx == 0)
        def _():
            copy_x(xb.at[7], xb.at[3], 3, 0, partner, sent_t).wait_send()

        @pl.when(dx == 1)
        def _():
            ref = xb.at[7, :, 0:N - KEPT]
            copy_x(ref, ref, 3, 0, partner, sent_t).wait_send()
            partial.wait_send()


SEMS = [
    pltpu.SemaphoreType.DMA((4,)),
    pltpu.SemaphoreType.DMA,
    pltpu.SemaphoreType.DMA,
    pltpu.SemaphoreType.DMA,
    pltpu.SemaphoreType.DMA,
    pltpu.SemaphoreType.DMA,
    pltpu.SemaphoreType.DMA((7, 2)),
    pltpu.SemaphoreType.DMA((7,)),
    pltpu.SemaphoreType.DMA((7,)),
    pltpu.SemaphoreType.DMA,
    pltpu.SemaphoreType.REGULAR,
    pltpu.SemaphoreType.REGULAR,
]


def kernel(*refs):
    pl.run_scoped(functools.partial(body, *refs), *SEMS)


def solution(mesh):
    spec = P(("dp", "team", "rep"), None)

    def per_device(points, values, pair_mask, bandwidth):
        hbm = [pltpu.with_memory_space_constraint(z, pltpu.HBM) for z in (points.T, values.T, pair_mask)]
        field = pl.pallas_call(
            kernel,
            out_shape=jax.ShapeDtypeStruct((1, N), jnp.float32),
            in_specs=[pl.BlockSpec(memory_space=pltpu.HBM)] * 3 + [pl.BlockSpec(memory_space=pltpu.SMEM)],
            out_specs=pl.BlockSpec(memory_space=pltpu.VMEM),
            scratch_shapes=[
                pltpu.VMEM((8, 88, N), jnp.bfloat16),
                pltpu.VMEM((8, 2, N), jnp.bfloat16),
                pltpu.VMEM((8, 1, N), jnp.bfloat16),
                pltpu.VMEM((4, 4), jnp.int32),
                pltpu.VMEM((96, N), jnp.bfloat16),
                pltpu.VMEM((16, N), jnp.float32),
                pltpu.VMEM((96, N), jnp.bfloat16),
                pltpu.VMEM((16, N), jnp.float32),
                pltpu.VMEM((1, N), jnp.float32),
                pltpu.VMEM((1, N), jnp.float32),
            ],
            compiler_params=pltpu.CompilerParams(collective_id=0, has_side_effects=True, vmem_limit_bytes=16 * 2**20),
        )(*hbm, bandwidth)
        return field.T

    return jax.shard_map(per_device, mesh=mesh, in_specs=(spec, spec, P("dp", None), P()), out_specs=spec, check_vma=False)
```

```python
import functools

import jax
import jax.numpy as jnp
from jax import lax
from jax.experimental import pallas as pl
from jax.experimental.pallas import tpu as pltpu
from jax.sharding import PartitionSpec as P

MESH = pl.DeviceIdType.MESH
N = 1024
LOG2E = 1.4426950408889634
WIDE = 2.0**64
TJ, TI, LAG = 512, 512, 1
HALVES = ((0, 512), (512, 512))
KEPT = 256


def split3(s):
    hi = s.astype(jnp.bfloat16).astype(jnp.float32)
    rest = s - hi
    mid = rest.astype(jnp.bfloat16).astype(jnp.float32)
    return hi, mid, rest - mid


def augment(xt, rest, scale=None):
    n = xt.shape[1]
    x32 = xt.astype(jnp.float32)
    r32 = rest.astype(jnp.float32)
    hi, mid, lo = split3(jnp.sum(x32 * x32, axis=0, keepdims=True) + jnp.sum(r32 * r32, axis=0, keepdims=True))
    last = jnp.concatenate([x32[80:88], r32, jnp.zeros((6, n), jnp.float32)], axis=0)
    row = lax.broadcasted_iota(jnp.int32, (16, n), 0)
    if scale is not None:
        tail = jnp.where(row < 10, -2.0 * last, jnp.where(row < 13, 1.0, jnp.where(row == 13, hi, jnp.where(row == 14, mid, lo))))
        return jnp.concatenate([(-2.0 * scale * x32[:80]).astype(jnp.bfloat16), (scale * tail).astype(jnp.bfloat16)], axis=0)
    tail = jnp.where(row < 10, last, jnp.where(row >= 13, 1.0, jnp.where(row == 10, hi, jnp.where(row == 11, mid, lo))))
    return jnp.concatenate([xt[:80], tail.astype(jnp.bfloat16)], axis=0)


def body(x_hbm, v_hbm, m_hbm, h_ref, o_ref, xb, rb, vb, mb, wb, fb, wp, fp, part_out, part_in, load_sem, sent_x, sent_r, sent_v, sent_t, sent_p, got_x, got_r, got_v, got_p, note, peer):
    y, t, dp = lax.axis_index("rep"), lax.axis_index("team"), lax.axis_index("dp")
    x, c = t // 2, t % 2
    dx = c + y - 2 * c * y
    odd = x + y - 2 * x * y
    first_chip, last_chip = (1 - x) * (1 - y), x * y

    def dev(fx, fy, fc):
        return (dp, y + fy - 2 * y * fy, 2 * (x + fx - 2 * x * fx) + c + fc - 2 * c * fc)

    def team_of(fx, fc):
        return 2 * (x + fx - 2 * x * fx) + c + fc - 2 * c * fc

    partner, target, source = dev(0, 0, 1), dev(dx, 1 - dx, dx), dev(1 - dx, dx, 1 - dx)

    def signal(sem, d):
        pl.semaphore_signal(sem, inc=1, device_id=d, device_id_type=MESH)

    bar = pltpu.get_barrier_semaphore()
    pl.when(last_chip == 0)(lambda: signal(bar, source))
    pl.when(jnp.maximum(c, 1 - odd) == 1)(lambda: signal(bar, partner))
    loads = [pltpu.make_async_copy(src, dst, load_sem.at[i]) for i, (src, dst) in enumerate(((x_hbm.at[0:88], xb.at[0]), (x_hbm.at[88:90], rb.at[0]), (v_hbm, vb.at[0]), (m_hbm, mb)))]

    def load():
        for z in loads:
            z.start()

    pl.when(first_chip == 1)(load)

    def copy_x(src, dst, slot, k, d, sent=sent_x):
        return pltpu.make_async_remote_copy(src_ref=src, dst_ref=dst, send_sem=sent, recv_sem=got_x.at[slot - 1, k], device_id=d, device_id_type=MESH)

    def copy_v(src, slot, d):
        return pltpu.make_async_remote_copy(src_ref=src, dst_ref=vb.at[slot], send_sem=sent_v, recv_sem=got_v.at[slot - 1], device_id=d, device_id_type=MESH)

    def copy_r(src, slot, d):
        return pltpu.make_async_remote_copy(src_ref=src, dst_ref=rb.at[slot], send_sem=sent_r, recv_sem=got_r.at[slot - 1], device_id=d, device_id_type=MESH)

    def send(x_src, r_src, v_src, slot, k, d, at=None, sent=sent_x):
        cols = pl.ds(*(at or HALVES[k]))
        if k == 0:
            copy_r(r_src, slot, d).start()
        copy_x(x_src.at[:, cols], xb.at[slot, :, cols], slot, k, d, sent).start()
        if k == 0:
            copy_v(v_src, slot, d).start()

    def pass_on(slot, to, k, d, at=None, sent=sent_x):
        send(xb.at[slot], rb.at[slot], vb.at[slot], to, k, d, at, sent)

    def arrive(slot, k, name, at=None):
        with jax.named_scope(f"{name}{k}"):
            if k == 0:
                copy_v(vb.at[slot], slot, partner).wait_recv()
                copy_r(rb.at[slot], slot, partner).wait_recv()
            ref = xb.at[slot, :, pl.ds(*(at or HALVES[k]))]
            copy_x(ref, ref, slot, k, partner).wait_recv()

    scale = jnp.where(h_ref[0] > WIDE, 1.0 / WIDE, 1.0)
    alpha = -LOG2E / (h_ref[0] * scale)

    def tiles(*parts, weights=wb, sums=fb):
        total, pend = {}, []

        def drain():
            i, vv, d = pend.pop(0)
            kern = jnp.exp2(d * alpha).astype(jnp.bfloat16)
            r = jnp.dot(vv, kern, preferred_element_type=jnp.float32)
            total[i] = total[i] + r if i in total else r

        with jax.named_scope("tiles"):
            for slot, team, at in parts:
                lhs = augment(xb[slot, :, at[0]:at[0] + at[1]], rb[slot, :, at[0]:at[0] + at[1]]).T
                for j in range(0, at[1], TJ):
                    size = min(TJ, at[1] - j)
                    rows = lax.broadcasted_iota(jnp.int32, (16, size), 0)
                    v32 = vb[slot, :, at[0] + j:at[0] + j + size].astype(jnp.float32)
                    vv = jnp.where(rows == team, jnp.broadcast_to(v32, (16, size)), 0.0).astype(jnp.bfloat16)
                    for i in range(0, N, TI):
                        pend.append((i, vv, jnp.dot(lhs[j:j + size], weights[:, i:i + TI], preferred_element_type=jnp.float32)))
                        if len(pend) > LAG:
                            drain()
            while pend:
                drain()
            for i in total:
                sums[:, i:i + TI] += total[i]

    def prepare():
        fb[...] = jnp.zeros_like(fb)
        for z in loads:
            z.wait()
        for i in range(0, N, 256):
            wb[:, i:i + 256] = augment(xb[0, :, i:i + 256], rb[0, :, i:i + 256], scale)

    def own_sum():
        tiles((0, team_of(0, 0), (0, N)))

    def own_to(slot, d):
        for k in range(2):
            send(x_hbm.at[0:88], x_hbm.at[88:90], v_hbm, slot, k, d)

    @pl.when(first_chip == 1)
    def _():
        prepare()
        own_sum()

    with jax.named_scope("bar"):
        pl.semaphore_wait(bar, 2 - odd)
    @pl.when(jnp.maximum(c, 1 - odd) == 1)
    def _():
        own_to(2 + 3 * dx, target)

    pl.when(last_chip == 1)(lambda: signal(peer, target))
    pl.when(odd * (1 - c) == 1)(lambda: signal(note, partner))
    pl.when(first_chip == 0)(load)

    @pl.when(odd * c == 1)
    def _():
        pl.semaphore_wait(note, 1)

    own_to(4, partner)

    @pl.when(first_chip == 0)
    def _():
        prepare()

    @pl.when(odd * c == 1)
    def _():
        with jax.named_scope("peer"):
            pl.semaphore_wait(peer, 1)
        signal(note, partner)

    @pl.when(odd * (1 - c) == 1)
    def _():
        with jax.named_scope("go"):
            pl.semaphore_wait(note, 1)
        own_to(2 + 3 * dx, target)

    for k in range(2):
        arrive(4, k, "own4_")
        pass_on(4, 6 - 5 * dx, k, target)

    pl.when(first_chip == 0)(own_sum)
    tiles((4, team_of(0, 1), (0, N)))
    def weight_of(team):
        mine = lax.broadcasted_iota(jnp.int32, (4, 4), 1) == team
        return jnp.sum(jnp.where(mine, mb[...].astype(jnp.float32), 0.0), axis=1, keepdims=True)

    weight = weight_of(t)

    @pl.when(dx == 1)
    def _():
        fp[...] = jnp.zeros_like(fp)
        for i in range(0, N, 256):
            wp[:, i:i + 256] = augment(xb[4, :, i:i + 256], rb[4, :, i:i + 256], scale)


    f1, f2, p1, p2 = 5 - 3 * dx, 1 + 5 * dx, 6 - 5 * dx, 2 + 3 * dx

    def first(k):
        arrive(f1, k, "f1_")
        pass_on(f1, 1 + 5 * dx, k, partner)
        pass_on(f1, 7, k, target)
        return f1, team_of(1 - dx, 1 - dx), HALVES[k]

    def second(k):
        arrive(f2, k, "f2_")
        pass_on(f2, 5 - 3 * dx, k, partner)
        return f2, team_of(1 - dx, dx), HALVES[k]

    def first_behind(k):
        arrive(p1, k, "p1_")
        return p1, team_of(dx, 1 - dx), HALVES[k]

    def second_behind(k):
        arrive(p2, k, "p2_")
        return p2, team_of(dx, dx), HALVES[k]

    direct, behind = (7, team_of(1, 1)), (3, team_of(1, 0))
    cut = (HALVES[1][0], HALVES[1][1] - KEPT)
    kept = (N - KEPT, KEPT)
    partial = pltpu.make_async_remote_copy(src_ref=part_out, dst_ref=part_in, send_sem=sent_p, recv_sem=got_p, device_id=partner, device_id_type=MESH)

    def third(k, at=None):
        arrive(7, k, "d7_")
        pass_on(7, 3, k, partner, at, sent_t)

    tiles(first(0))
    tiles(first(1), first_behind(0))
    tiles(second(0), first_behind(1))

    def lead():
        tiles(second(1), second_behind(0))
        third(0)
        tiles((*direct, HALVES[0]), second_behind(1))

    @pl.when(dx == 0)
    def _():
        lead()
        third(1)
        arrive(3, 0, "d3_")
        tiles((*direct, HALVES[1]), (*behind, HALVES[0]))
        arrive(3, 1, "d3_", cut)
        tiles((*behind, cut))
        partial.wait_recv()
        o_ref[...] = jnp.sum(fb[0:4] * weight, axis=0, keepdims=True) + part_in[...]

    @pl.when(dx == 1)
    def _():
        lead()
        third(1, cut)
        tiles((*direct, kept), weights=wp, sums=fp)
        part_out[...] = jnp.sum(fp[0:4] * weight_of(team_of(0, 1)), axis=0, keepdims=True)
        arrive(3, 0, "d3_")
        partial.start()
        tiles((*direct, HALVES[1]), (*behind, HALVES[0]))
        arrive(3, 1, "d3_")
        tiles((*behind, HALVES[1]))
        o_ref[...] = jnp.sum(fb[0:4] * weight, axis=0, keepdims=True)

    with jax.named_scope("sendw"):
        copy_x(xb.at[0:6], xb.at[1:7], 1, 0, partner).wait_send()
        pltpu.make_async_remote_copy(src_ref=rb.at[0:7], dst_ref=rb.at[1:8], send_sem=sent_r, recv_sem=got_r.at[0], device_id=partner, device_id_type=MESH).wait_send()
        copy = pltpu.make_async_remote_copy(src_ref=vb.at[0:7], dst_ref=vb.at[1:8], send_sem=sent_v, recv_sem=got_v.at[0], device_id=partner, device_id_type=MESH)
        copy.wait_send()

        @pl.when(dx == 0)
        def _():
            copy_x(xb.at[7], xb.at[3], 3, 0, partner, sent_t).wait_send()

        @pl.when(dx == 1)
        def _():
            ref = xb.at[7, :, 0:N - KEPT]
            copy_x(ref, ref, 3, 0, partner, sent_t).wait_send()
            partial.wait_send()


SEMS = [
    pltpu.SemaphoreType.DMA((4,)),
    pltpu.SemaphoreType.DMA,
    pltpu.SemaphoreType.DMA,
    pltpu.SemaphoreType.DMA,
    pltpu.SemaphoreType.DMA,
    pltpu.SemaphoreType.DMA,
    pltpu.SemaphoreType.DMA((7, 2)),
    pltpu.SemaphoreType.DMA((7,)),
    pltpu.SemaphoreType.DMA((7,)),
    pltpu.SemaphoreType.DMA,
    pltpu.SemaphoreType.REGULAR,
    pltpu.SemaphoreType.REGULAR,
]


def kernel(*refs):
    pl.run_scoped(functools.partial(body, *refs), *SEMS)


def solution(mesh):
    spec = P(("dp", "team", "rep"), None)

    def per_device(points, values, pair_mask, bandwidth):
        hbm = [pltpu.with_memory_space_constraint(z, pltpu.HBM) for z in (points.T, values.T, pair_mask)]
        field = pl.pallas_call(
            kernel,
            out_shape=jax.ShapeDtypeStruct((1, N), jnp.float32),
            in_specs=[pl.BlockSpec(memory_space=pltpu.HBM)] * 3 + [pl.BlockSpec(memory_space=pltpu.SMEM)],
            out_specs=pl.BlockSpec(memory_space=pltpu.VMEM),
            scratch_shapes=[
                pltpu.VMEM((8, 88, N), jnp.bfloat16),
                pltpu.VMEM((8, 2, N), jnp.bfloat16),
                pltpu.VMEM((8, 1, N), jnp.bfloat16),
                pltpu.VMEM((4, 4), jnp.int32),
                pltpu.VMEM((96, N), jnp.bfloat16),
                pltpu.VMEM((16, N), jnp.float32),
                pltpu.VMEM((96, N), jnp.bfloat16),
                pltpu.VMEM((16, N), jnp.float32),
                pltpu.VMEM((1, N), jnp.float32),
                pltpu.VMEM((1, N), jnp.float32),
            ],
            compiler_params=pltpu.CompilerParams(collective_id=0, has_side_effects=True, vmem_limit_bytes=16 * 2**20),
        )(*hbm, bandwidth)
        return field.T

    return jax.shard_map(per_device, mesh=mesh, in_specs=(spec, spec, P("dp", None), P()), out_specs=spec, check_vma=False)
```

```python
import functools

import jax
import jax.numpy as jnp
from jax import lax
from jax.experimental import pallas as pl
from jax.experimental.pallas import tpu as pltpu
from jax.sharding import PartitionSpec as P

MESH = pl.DeviceIdType.MESH
N = 1024
LOG2E = 1.4426950408889634
WIDE = 2.0**64
TJ, TI, LAG = 512, 512, 1
HALVES = ((0, 512), (512, 512))
KEPT = 256


def split3(s):
    hi = s.astype(jnp.bfloat16).astype(jnp.float32)
    rest = s - hi
    mid = rest.astype(jnp.bfloat16).astype(jnp.float32)
    return hi, mid, rest - mid


def augment(xt, rest, scale=None):
    n = xt.shape[1]
    x32 = xt.astype(jnp.float32)
    r32 = rest.astype(jnp.float32)
    hi, mid, lo = split3(jnp.sum(x32 * x32, axis=0, keepdims=True) + jnp.sum(r32 * r32, axis=0, keepdims=True))
    last = jnp.concatenate([x32[80:88], r32, jnp.zeros((6, n), jnp.float32)], axis=0)
    row = lax.broadcasted_iota(jnp.int32, (16, n), 0)
    if scale is not None:
        tail = jnp.where(row < 10, -2.0 * last, jnp.where(row < 13, 1.0, jnp.where(row == 13, hi, jnp.where(row == 14, mid, lo))))
        return jnp.concatenate([(-2.0 * scale * x32[:80]).astype(jnp.bfloat16), (scale * tail).astype(jnp.bfloat16)], axis=0)
    tail = jnp.where(row < 10, last, jnp.where(row >= 13, 1.0, jnp.where(row == 10, hi, jnp.where(row == 11, mid, lo))))
    return jnp.concatenate([xt[:80], tail.astype(jnp.bfloat16)], axis=0)


def body(x_hbm, v_hbm, m_hbm, h_ref, o_ref, xb, rb, vb, mb, wb, fb, wp, fp, part_out, part_in, load_sem, sent_x, sent_r, sent_v, sent_t, sent_p, got_x, got_r, got_v, got_p, note, peer):
    y, t, dp = lax.axis_index("rep"), lax.axis_index("team"), lax.axis_index("dp")
    x, c = t // 2, t % 2
    dx = c + y - 2 * c * y
    odd = x + y - 2 * x * y
    first_chip, last_chip = (1 - x) * (1 - y), x * y

    def dev(fx, fy, fc):
        return (dp, y + fy - 2 * y * fy, 2 * (x + fx - 2 * x * fx) + c + fc - 2 * c * fc)

    def team_of(fx, fc):
        return 2 * (x + fx - 2 * x * fx) + c + fc - 2 * c * fc

    partner, target, source = dev(0, 0, 1), dev(dx, 1 - dx, dx), dev(1 - dx, dx, 1 - dx)

    def signal(sem, d):
        pl.semaphore_signal(sem, inc=1, device_id=d, device_id_type=MESH)

    bar = pltpu.get_barrier_semaphore()
    pl.when(odd * c == 1)(lambda: signal(bar, source))
    pl.when(odd == 0)(lambda: signal(bar, partner))
    loads = [pltpu.make_async_copy(src, dst, load_sem.at[i]) for i, (src, dst) in enumerate(((x_hbm.at[0:88], xb.at[0]), (x_hbm.at[88:90], rb.at[0]), (v_hbm, vb.at[0]), (m_hbm, mb)))]

    def load():
        for z in loads:
            z.start()

    pl.when(first_chip == 1)(load)

    def copy_x(src, dst, slot, k, d, sent=sent_x):
        return pltpu.make_async_remote_copy(src_ref=src, dst_ref=dst, send_sem=sent, recv_sem=got_x.at[slot - 1, k], device_id=d, device_id_type=MESH)

    def copy_v(src, slot, d):
        return pltpu.make_async_remote_copy(src_ref=src, dst_ref=vb.at[slot], send_sem=sent_v, recv_sem=got_v.at[slot - 1], device_id=d, device_id_type=MESH)

    def copy_r(src, slot, d):
        return pltpu.make_async_remote_copy(src_ref=src, dst_ref=rb.at[slot], send_sem=sent_r, recv_sem=got_r.at[slot - 1], device_id=d, device_id_type=MESH)

    def send(x_src, r_src, v_src, slot, k, d, at=None, sent=sent_x):
        cols = pl.ds(*(at or HALVES[k]))
        if k == 0:
            copy_r(r_src, slot, d).start()
        copy_x(x_src.at[:, cols], xb.at[slot, :, cols], slot, k, d, sent).start()
        if k == 0:
            copy_v(v_src, slot, d).start()

    def pass_on(slot, to, k, d, at=None, sent=sent_x):
        send(xb.at[slot], rb.at[slot], vb.at[slot], to, k, d, at, sent)

    def arrive(slot, k, name, at=None):
        with jax.named_scope(f"{name}{k}"):
            if k == 0:
                copy_v(vb.at[slot], slot, partner).wait_recv()
                copy_r(rb.at[slot], slot, partner).wait_recv()
            ref = xb.at[slot, :, pl.ds(*(at or HALVES[k]))]
            copy_x(ref, ref, slot, k, partner).wait_recv()

    scale = jnp.where(h_ref[0] > WIDE, 1.0 / WIDE, 1.0)
    alpha = -LOG2E / (h_ref[0] * scale)

    def tiles(*parts, weights=wb, sums=fb):
        total, pend = {}, []

        def drain():
            i, vv, d = pend.pop(0)
            kern = jnp.exp2(d * alpha).astype(jnp.bfloat16)
            r = jnp.dot(vv, kern, preferred_element_type=jnp.float32)
            total[i] = total[i] + r if i in total else r

        with jax.named_scope("tiles"):
            for slot, team, at in parts:
                lhs = augment(xb[slot, :, at[0]:at[0] + at[1]], rb[slot, :, at[0]:at[0] + at[1]]).T
                for j in range(0, at[1], TJ):
                    size = min(TJ, at[1] - j)
                    rows = lax.broadcasted_iota(jnp.int32, (16, size), 0)
                    v32 = vb[slot, :, at[0] + j:at[0] + j + size].astype(jnp.float32)
                    vv = jnp.where(rows == team, jnp.broadcast_to(v32, (16, size)), 0.0).astype(jnp.bfloat16)
                    for i in range(0, N, TI):
                        pend.append((i, vv, jnp.dot(lhs[j:j + size], weights[:, i:i + TI], preferred_element_type=jnp.float32)))
                        if len(pend) > LAG:
                            drain()
            while pend:
                drain()
            for i in total:
                sums[:, i:i + TI] += total[i]

    def prepare():
        fb[...] = jnp.zeros_like(fb)
        for z in loads:
            z.wait()
        for i in range(0, N, 256):
            wb[:, i:i + 256] = augment(xb[0, :, i:i + 256], rb[0, :, i:i + 256], scale)

    def own_sum():
        tiles((0, team_of(0, 0), (0, N)))

    def own_to(slot, d):
        for k in range(2):
            send(x_hbm.at[0:88], x_hbm.at[88:90], v_hbm, slot, k, d)

    with jax.named_scope("bar"):
        pl.semaphore_wait(bar, 1 + last_chip)

    def pass_partner(wait):
        for k in range(2):
            if wait:
                arrive(4, k, "own4_")
            pass_on(4, 6 - 5 * dx, k, target)

    def part_sum():
        tiles((4, team_of(0, 1), (0, N)))

    @pl.when(first_chip == 1)
    def _():
        signal(bar, source)
        own_to(4, partner)
        prepare()
        own_sum()
        for k in range(2):
            arrive(4, k, "own4_")
        part_sum()
        with jax.named_scope("peer"):
            pl.semaphore_wait(peer, 1)
        own_to(2 + 3 * dx, target)
        pass_partner(False)

    @pl.when(jnp.maximum(odd * c, last_chip) == 1)
    def _():
        own_to(2 + 3 * dx, target)

    @pl.when(odd * c == 1)
    def _():
        signal(bar, partner)

    pl.when(last_chip == 1)(lambda: signal(peer, target))

    @pl.when(odd * (1 - c) == 1)
    def _():
        signal(note, partner)
        signal(peer, source)

    @pl.when(first_chip == 0)
    def _():
        load()

        @pl.when(odd * c == 1)
        def _():
            pl.semaphore_wait(note, 1)

        own_to(4, partner)
        prepare()

        @pl.when(odd * c == 1)
        def _():
            with jax.named_scope("peer"):
                pl.semaphore_wait(peer, 1)
            signal(note, partner)

        @pl.when(odd * (1 - c) == 1)
        def _():
            with jax.named_scope("go"):
                pl.semaphore_wait(note, 1)
            own_to(2 + 3 * dx, target)

        pass_partner(True)
        own_sum()
        part_sum()

    def weight_of(team):
        mine = lax.broadcasted_iota(jnp.int32, (4, 4), 1) == team
        return jnp.sum(jnp.where(mine, mb[...].astype(jnp.float32), 0.0), axis=1, keepdims=True)

    weight = weight_of(t)

    @pl.when(dx == 1)
    def _():
        fp[...] = jnp.zeros_like(fp)
        for i in range(0, N, 256):
            wp[:, i:i + 256] = augment(xb[4, :, i:i + 256], rb[4, :, i:i + 256], scale)


    f1, f2, p1, p2 = 5 - 3 * dx, 1 + 5 * dx, 6 - 5 * dx, 2 + 3 * dx

    def first(k):
        arrive(f1, k, "f1_")
        pass_on(f1, 1 + 5 * dx, k, partner)
        pass_on(f1, 7, k, target)
        return f1, team_of(1 - dx, 1 - dx), HALVES[k]

    def second(k):
        arrive(f2, k, "f2_")
        pass_on(f2, 5 - 3 * dx, k, partner)
        return f2, team_of(1 - dx, dx), HALVES[k]

    def first_behind(k):
        arrive(p1, k, "p1_")
        return p1, team_of(dx, 1 - dx), HALVES[k]

    def second_behind(k):
        arrive(p2, k, "p2_")
        return p2, team_of(dx, dx), HALVES[k]

    direct, behind = (7, team_of(1, 1)), (3, team_of(1, 0))
    cut = (HALVES[1][0], HALVES[1][1] - KEPT)
    kept = (N - KEPT, KEPT)
    partial = pltpu.make_async_remote_copy(src_ref=part_out, dst_ref=part_in, send_sem=sent_p, recv_sem=got_p, device_id=partner, device_id_type=MESH)

    def third(k, at=None):
        arrive(7, k, "d7_")
        pass_on(7, 3, k, partner, at, sent_t)

    tiles(first(0))
    tiles(first(1), first_behind(0))
    tiles(second(0), first_behind(1))

    def lead():
        tiles(second(1), second_behind(0))
        third(0)
        tiles((*direct, HALVES[0]), second_behind(1))

    @pl.when(dx == 0)
    def _():
        lead()
        third(1)
        arrive(3, 0, "d3_")
        tiles((*direct, HALVES[1]), (*behind, HALVES[0]))
        arrive(3, 1, "d3_", cut)
        tiles((*behind, cut))
        partial.wait_recv()
        o_ref[...] = jnp.sum(fb[0:4] * weight, axis=0, keepdims=True) + part_in[...]

    @pl.when(dx == 1)
    def _():
        lead()
        third(1, cut)
        tiles((*direct, kept), weights=wp, sums=fp)
        part_out[...] = jnp.sum(fp[0:4] * weight_of(team_of(0, 1)), axis=0, keepdims=True)
        arrive(3, 0, "d3_")
        partial.start()
        tiles((*direct, HALVES[1]), (*behind, HALVES[0]))
        arrive(3, 1, "d3_")
        tiles((*behind, HALVES[1]))
        o_ref[...] = jnp.sum(fb[0:4] * weight, axis=0, keepdims=True)

    with jax.named_scope("sendw"):
        copy_x(xb.at[0:6], xb.at[1:7], 1, 0, partner).wait_send()
        pltpu.make_async_remote_copy(src_ref=rb.at[0:7], dst_ref=rb.at[1:8], send_sem=sent_r, recv_sem=got_r.at[0], device_id=partner, device_id_type=MESH).wait_send()
        copy = pltpu.make_async_remote_copy(src_ref=vb.at[0:7], dst_ref=vb.at[1:8], send_sem=sent_v, recv_sem=got_v.at[0], device_id=partner, device_id_type=MESH)
        copy.wait_send()

        @pl.when(dx == 0)
        def _():
            copy_x(xb.at[7], xb.at[3], 3, 0, partner, sent_t).wait_send()

        @pl.when(dx == 1)
        def _():
            ref = xb.at[7, :, 0:N - KEPT]
            copy_x(ref, ref, 3, 0, partner, sent_t).wait_send()
            partial.wait_send()


SEMS = [
    pltpu.SemaphoreType.DMA((4,)),
    pltpu.SemaphoreType.DMA,
    pltpu.SemaphoreType.DMA,
    pltpu.SemaphoreType.DMA,
    pltpu.SemaphoreType.DMA,
    pltpu.SemaphoreType.DMA,
    pltpu.SemaphoreType.DMA((7, 2)),
    pltpu.SemaphoreType.DMA((7,)),
    pltpu.SemaphoreType.DMA((7,)),
    pltpu.SemaphoreType.DMA,
    pltpu.SemaphoreType.REGULAR,
    pltpu.SemaphoreType.REGULAR,
]


def kernel(*refs):
    pl.run_scoped(functools.partial(body, *refs), *SEMS)


def solution(mesh):
    spec = P(("dp", "team", "rep"), None)

    def per_device(points, values, pair_mask, bandwidth):
        hbm = [pltpu.with_memory_space_constraint(z, pltpu.HBM) for z in (points.T, values.T, pair_mask)]
        field = pl.pallas_call(
            kernel,
            out_shape=jax.ShapeDtypeStruct((1, N), jnp.float32),
            in_specs=[pl.BlockSpec(memory_space=pltpu.HBM)] * 3 + [pl.BlockSpec(memory_space=pltpu.SMEM)],
            out_specs=pl.BlockSpec(memory_space=pltpu.VMEM),
            scratch_shapes=[
                pltpu.VMEM((8, 88, N), jnp.bfloat16),
                pltpu.VMEM((8, 2, N), jnp.bfloat16),
                pltpu.VMEM((8, 1, N), jnp.bfloat16),
                pltpu.VMEM((4, 4), jnp.int32),
                pltpu.VMEM((96, N), jnp.bfloat16),
                pltpu.VMEM((16, N), jnp.float32),
                pltpu.VMEM((96, N), jnp.bfloat16),
                pltpu.VMEM((16, N), jnp.float32),
                pltpu.VMEM((1, N), jnp.float32),
                pltpu.VMEM((1, N), jnp.float32),
            ],
            compiler_params=pltpu.CompilerParams(collective_id=0, has_side_effects=True, vmem_limit_bytes=16 * 2**20),
        )(*hbm, bandwidth)
        return field.T

    return jax.shard_map(per_device, mesh=mesh, in_specs=(spec, spec, P("dp", None), P()), out_specs=spec, check_vma=False)
```

```python
import functools

import jax
import jax.numpy as jnp
from jax import lax
from jax.experimental import pallas as pl
from jax.experimental.pallas import tpu as pltpu
from jax.sharding import PartitionSpec as P

MESH = pl.DeviceIdType.MESH
N = 1024
LOG2E = 1.4426950408889634
WIDE = 2.0**64
TJ, TI, LAG = 512, 512, 1
HALVES = ((0, 512), (512, 512))
KEPT = 256


def split3(s):
    hi = s.astype(jnp.bfloat16).astype(jnp.float32)
    rest = s - hi
    mid = rest.astype(jnp.bfloat16).astype(jnp.float32)
    return hi, mid, rest - mid


def augment(xt, rest, scale=None):
    n = xt.shape[1]
    x32 = xt.astype(jnp.float32)
    r32 = rest.astype(jnp.float32)
    hi, mid, lo = split3(jnp.sum(x32 * x32, axis=0, keepdims=True) + jnp.sum(r32 * r32, axis=0, keepdims=True))
    last = jnp.concatenate([x32[80:88], r32, jnp.zeros((6, n), jnp.float32)], axis=0)
    row = lax.broadcasted_iota(jnp.int32, (16, n), 0)
    if scale is not None:
        tail = jnp.where(row < 10, -2.0 * last, jnp.where(row < 13, 1.0, jnp.where(row == 13, hi, jnp.where(row == 14, mid, lo))))
        return jnp.concatenate([(-2.0 * scale * x32[:80]).astype(jnp.bfloat16), (scale * tail).astype(jnp.bfloat16)], axis=0)
    tail = jnp.where(row < 10, last, jnp.where(row >= 13, 1.0, jnp.where(row == 10, hi, jnp.where(row == 11, mid, lo))))
    return jnp.concatenate([xt[:80], tail.astype(jnp.bfloat16)], axis=0)


def body(x_hbm, v_hbm, m_hbm, h_ref, o_ref, xb, rb, vb, mb, wb, fb, wp, fp, part_out, part_in, load_sem, sent_x, sent_r, sent_v, sent_t, sent_p, got_x, got_r, got_v, got_p, note, peer):
    y, t, dp = lax.axis_index("rep"), lax.axis_index("team"), lax.axis_index("dp")
    x, c = t // 2, t % 2
    dx = c + y - 2 * c * y
    odd = x + y - 2 * x * y
    first_chip, last_chip = (1 - x) * (1 - y), x * y

    def dev(fx, fy, fc):
        return (dp, y + fy - 2 * y * fy, 2 * (x + fx - 2 * x * fx) + c + fc - 2 * c * fc)

    def team_of(fx, fc):
        return 2 * (x + fx - 2 * x * fx) + c + fc - 2 * c * fc

    partner, target, source = dev(0, 0, 1), dev(dx, 1 - dx, dx), dev(1 - dx, dx, 1 - dx)

    def signal(sem, d):
        pl.semaphore_signal(sem, inc=1, device_id=d, device_id_type=MESH)

    bar = pltpu.get_barrier_semaphore()
    pl.when(odd * c == 1)(lambda: signal(bar, source))
    pl.when(odd == 0)(lambda: signal(bar, partner))
    loads = [pltpu.make_async_copy(src, dst, load_sem.at[i]) for i, (src, dst) in enumerate(((x_hbm.at[0:88], xb.at[0]), (x_hbm.at[88:90], rb.at[0]), (v_hbm, vb.at[0]), (m_hbm, mb)))]

    def load():
        for z in loads:
            z.start()

    pl.when(first_chip == 1)(load)

    def copy_x(src, dst, slot, k, d, sent=sent_x):
        return pltpu.make_async_remote_copy(src_ref=src, dst_ref=dst, send_sem=sent, recv_sem=got_x.at[slot - 1, k], device_id=d, device_id_type=MESH)

    def copy_v(src, slot, d):
        return pltpu.make_async_remote_copy(src_ref=src, dst_ref=vb.at[slot], send_sem=sent_v, recv_sem=got_v.at[slot - 1], device_id=d, device_id_type=MESH)

    def copy_r(src, slot, d):
        return pltpu.make_async_remote_copy(src_ref=src, dst_ref=rb.at[slot], send_sem=sent_r, recv_sem=got_r.at[slot - 1], device_id=d, device_id_type=MESH)

    def send(x_src, r_src, v_src, slot, k, d, at=None, sent=sent_x):
        cols = pl.ds(*(at or HALVES[k]))
        if k == 0:
            copy_r(r_src, slot, d).start()
        copy_x(x_src.at[:, cols], xb.at[slot, :, cols], slot, k, d, sent).start()
        if k == 0:
            copy_v(v_src, slot, d).start()

    def pass_on(slot, to, k, d, at=None, sent=sent_x):
        send(xb.at[slot], rb.at[slot], vb.at[slot], to, k, d, at, sent)

    def arrive(slot, k, name, at=None):
        with jax.named_scope(f"{name}{k}"):
            if k == 0:
                copy_v(vb.at[slot], slot, partner).wait_recv()
                copy_r(rb.at[slot], slot, partner).wait_recv()
            ref = xb.at[slot, :, pl.ds(*(at or HALVES[k]))]
            copy_x(ref, ref, slot, k, partner).wait_recv()

    scale = jnp.where(h_ref[0] > WIDE, 1.0 / WIDE, 1.0)
    alpha = -LOG2E / (h_ref[0] * scale)

    def tiles(*parts, weights=wb, sums=fb):
        total, pend = {}, []

        def drain():
            i, vv, d = pend.pop(0)
            kern = jnp.exp2(d * alpha).astype(jnp.bfloat16)
            r = jnp.dot(vv, kern, preferred_element_type=jnp.float32)
            total[i] = total[i] + r if i in total else r

        with jax.named_scope("tiles"):
            for slot, team, at in parts:
                lhs = augment(xb[slot, :, at[0]:at[0] + at[1]], rb[slot, :, at[0]:at[0] + at[1]]).T
                for j in range(0, at[1], TJ):
                    size = min(TJ, at[1] - j)
                    rows = lax.broadcasted_iota(jnp.int32, (16, size), 0)
                    v32 = vb[slot, :, at[0] + j:at[0] + j + size].astype(jnp.float32)
                    vv = jnp.where(rows == team, jnp.broadcast_to(v32, (16, size)), 0.0).astype(jnp.bfloat16)
                    for i in range(0, N, TI):
                        pend.append((i, vv, jnp.dot(lhs[j:j + size], weights[:, i:i + TI], preferred_element_type=jnp.float32)))
                        if len(pend) > LAG:
                            drain()
            while pend:
                drain()
            for i in total if sums is not None else ():
                sums[:, i:i + TI] += total[i]
        return total

    def prepare():
        fb[...] = jnp.zeros_like(fb)
        for z in loads:
            z.wait()
        for i in range(0, N, 256):
            wb[:, i:i + 256] = augment(xb[0, :, i:i + 256], rb[0, :, i:i + 256], scale)

    def own_sum():
        tiles((0, team_of(0, 0), (0, N)))

    def own_to(slot, d):
        for k in range(2):
            send(x_hbm.at[0:88], x_hbm.at[88:90], v_hbm, slot, k, d)

    with jax.named_scope("bar"):
        pl.semaphore_wait(bar, 1 + last_chip)

    def pass_partner(wait):
        for k in range(2):
            if wait:
                arrive(4, k, "own4_")
            pass_on(4, 6 - 5 * dx, k, target)

    def part_sum():
        tiles((4, team_of(0, 1), (0, N)))

    @pl.when(first_chip == 1)
    def _():
        signal(bar, source)
        own_to(4, partner)
        prepare()
        own_sum()
        for k in range(2):
            arrive(4, k, "own4_")
        part_sum()
        with jax.named_scope("peer"):
            pl.semaphore_wait(peer, 1)
        own_to(2 + 3 * dx, target)
        pass_partner(False)

    @pl.when(jnp.maximum(odd * c, last_chip) == 1)
    def _():
        own_to(2 + 3 * dx, target)

    @pl.when(odd * c == 1)
    def _():
        signal(bar, partner)

    pl.when(last_chip == 1)(lambda: signal(peer, target))

    @pl.when(odd * (1 - c) == 1)
    def _():
        signal(note, partner)
        signal(peer, source)

    @pl.when(first_chip == 0)
    def _():
        load()

        @pl.when(odd * c == 1)
        def _():
            pl.semaphore_wait(note, 1)

        own_to(4, partner)
        prepare()

        @pl.when(odd * c == 1)
        def _():
            with jax.named_scope("peer"):
                pl.semaphore_wait(peer, 1)
            signal(note, partner)

        @pl.when(odd * (1 - c) == 1)
        def _():
            with jax.named_scope("go"):
                pl.semaphore_wait(note, 1)
            own_to(2 + 3 * dx, target)

        pass_partner(True)
        own_sum()
        part_sum()

    def weight_of(team):
        mine = lax.broadcasted_iota(jnp.int32, (4, 4), 1) == team
        return jnp.sum(jnp.where(mine, mb[...].astype(jnp.float32), 0.0), axis=1, keepdims=True)

    weight = weight_of(t)

    @pl.when(dx == 1)
    def _():
        fp[...] = jnp.zeros_like(fp)
        for i in range(0, N, 256):
            wp[:, i:i + 256] = augment(xb[4, :, i:i + 256], rb[4, :, i:i + 256], scale)


    f1, f2, p1, p2 = 5 - 3 * dx, 1 + 5 * dx, 6 - 5 * dx, 2 + 3 * dx

    def first(k):
        arrive(f1, k, "f1_")
        pass_on(f1, 1 + 5 * dx, k, partner)
        pass_on(f1, 7, k, target)
        return f1, team_of(1 - dx, 1 - dx), HALVES[k]

    def second(k):
        arrive(f2, k, "f2_")
        pass_on(f2, 5 - 3 * dx, k, partner)
        return f2, team_of(1 - dx, dx), HALVES[k]

    def first_behind(k):
        arrive(p1, k, "p1_")
        return p1, team_of(dx, 1 - dx), HALVES[k]

    def second_behind(k):
        arrive(p2, k, "p2_")
        return p2, team_of(dx, dx), HALVES[k]

    direct, behind = (7, team_of(1, 1)), (3, team_of(1, 0))
    cut = (HALVES[1][0], HALVES[1][1] - KEPT)
    kept = (N - KEPT, KEPT)
    partial = pltpu.make_async_remote_copy(src_ref=part_out, dst_ref=part_in, send_sem=sent_p, recv_sem=got_p, device_id=partner, device_id_type=MESH)

    def third(k, at=None):
        arrive(7, k, "d7_")
        pass_on(7, 3, k, partner, at, sent_t)

    tiles(first(0))
    tiles(first(1), first_behind(0))
    tiles(second(0), first_behind(1))

    def lead():
        tiles(second(1), second_behind(0))
        third(0)
        tiles((*direct, HALVES[0]), second_behind(1))

    @pl.when(dx == 0)
    def _():
        lead()
        third(1)
        arrive(3, 0, "d3_")
        tiles((*direct, HALVES[1]), (*behind, HALVES[0]))
        arrive(3, 1, "d3_", cut)
        tiles((*behind, cut))
        partial.wait_recv()
        o_ref[...] = jnp.sum(fb[0:4] * weight, axis=0, keepdims=True) + part_in[...]

    @pl.when(dx == 1)
    def _():
        lead()
        third(1, cut)
        ours = tiles((*direct, kept), weights=wp, sums=None)
        partner_weight = weight_of(team_of(0, 1))
        for i in ours:
            part_out[:, i:i + TI] = jnp.sum(ours[i][0:4] * partner_weight, axis=0, keepdims=True)
        arrive(3, 0, "d3_")
        partial.start()
        tiles((*direct, HALVES[1]), (*behind, HALVES[0]))
        arrive(3, 1, "d3_")
        tiles((*behind, HALVES[1]))
        o_ref[...] = jnp.sum(fb[0:4] * weight, axis=0, keepdims=True)

    with jax.named_scope("sendw"):
        copy_x(xb.at[0:6], xb.at[1:7], 1, 0, partner).wait_send()
        pltpu.make_async_remote_copy(src_ref=rb.at[0:7], dst_ref=rb.at[1:8], send_sem=sent_r, recv_sem=got_r.at[0], device_id=partner, device_id_type=MESH).wait_send()
        copy = pltpu.make_async_remote_copy(src_ref=vb.at[0:7], dst_ref=vb.at[1:8], send_sem=sent_v, recv_sem=got_v.at[0], device_id=partner, device_id_type=MESH)
        copy.wait_send()

        @pl.when(dx == 0)
        def _():
            copy_x(xb.at[7], xb.at[3], 3, 0, partner, sent_t).wait_send()

        @pl.when(dx == 1)
        def _():
            ref = xb.at[7, :, 0:N - KEPT]
            copy_x(ref, ref, 3, 0, partner, sent_t).wait_send()
            partial.wait_send()


SEMS = [
    pltpu.SemaphoreType.DMA((4,)),
    pltpu.SemaphoreType.DMA,
    pltpu.SemaphoreType.DMA,
    pltpu.SemaphoreType.DMA,
    pltpu.SemaphoreType.DMA,
    pltpu.SemaphoreType.DMA,
    pltpu.SemaphoreType.DMA((7, 2)),
    pltpu.SemaphoreType.DMA((7,)),
    pltpu.SemaphoreType.DMA((7,)),
    pltpu.SemaphoreType.DMA,
    pltpu.SemaphoreType.REGULAR,
    pltpu.SemaphoreType.REGULAR,
]


def kernel(*refs):
    pl.run_scoped(functools.partial(body, *refs), *SEMS)


def solution(mesh):
    spec = P(("dp", "team", "rep"), None)

    def per_device(points, values, pair_mask, bandwidth):
        hbm = [pltpu.with_memory_space_constraint(z, pltpu.HBM) for z in (points.T, values.T, pair_mask)]
        field = pl.pallas_call(
            kernel,
            out_shape=jax.ShapeDtypeStruct((1, N), jnp.float32),
            in_specs=[pl.BlockSpec(memory_space=pltpu.HBM)] * 3 + [pl.BlockSpec(memory_space=pltpu.SMEM)],
            out_specs=pl.BlockSpec(memory_space=pltpu.VMEM),
            scratch_shapes=[
                pltpu.VMEM((8, 88, N), jnp.bfloat16),
                pltpu.VMEM((8, 2, N), jnp.bfloat16),
                pltpu.VMEM((8, 1, N), jnp.bfloat16),
                pltpu.VMEM((4, 4), jnp.int32),
                pltpu.VMEM((96, N), jnp.bfloat16),
                pltpu.VMEM((16, N), jnp.float32),
                pltpu.VMEM((96, N), jnp.bfloat16),
                pltpu.VMEM((16, N), jnp.float32),
                pltpu.VMEM((1, N), jnp.float32),
                pltpu.VMEM((1, N), jnp.float32),
            ],
            compiler_params=pltpu.CompilerParams(collective_id=0, has_side_effects=True, vmem_limit_bytes=16 * 2**20),
        )(*hbm, bandwidth)
        return field.T

    return jax.shard_map(per_device, mesh=mesh, in_specs=(spec, spec, P("dp", None), P()), out_specs=spec, check_vma=False)
```
